8 devices in a mesh: dp: 1 (over z), tp: 8 (over y, x, core).
Axes of the slice: x: 2, y: 2, z: 1, core: 2. Of those that a mesh axis runs over, the one named last changes fastest.
Arguments:
- hidden: bfloat16 [1, 512, 2560], P('dp')
- norm_w: bfloat16 [2, 2560], replicated
- w_z: bfloat16 [2, 2560, 5120], P(None, None, 'tp')
- w_x: bfloat16 [2, 2560, 5120], P(None, None, 'tp')
- w_bc: bfloat16 [2, 2560, 128], replicated
- w_dt: bfloat16 [2, 2560, 80], P(None, None, 'tp')
- conv_x: bfloat16 [2, 4, 5120], P(None, None, 'tp')
- conv_bc: bfloat16 [2, 4, 128], replicated
- bias_x: bfloat16 [2, 5120], P(None, 'tp')
- bias_bc: bfloat16 [2, 128], replicated
- dt_bias: float32 [2, 80], P(None, 'tp')
- a_log: float32 [2, 80], P(None, 'tp')
- d_skip: float32 [2, 80], P(None, 'tp')
- gate_w: bfloat16 [2, 5120], P(None, 'tp')
- w_out: bfloat16 [2, 5120, 2560], P(None, 'tp')
Outputs:
- output: bfloat16 [1, 512, 2560], P('dp')
All inputs are finite; a program needn't handle non-finite values.
Results may differ from the reference program's by a relative error of at most 0.0144688.
Values sent between devices are 32-bit elements.
A program may use at most 1 GiB of HBM per device.

```python
import math
import jax
import jax.numpy as jnp
from jax import lax

BATCH_ROWS = 1
SEQ_LEN = 512
D_MODEL = 2560
HEADS = 80
HEAD_DIM = 64
STATE_DIM = 64
LAYERS = 2
CONV_WIDTH = 4
BLOCK_LEN = 256

INNER_WIDTH = HEADS * HEAD_DIM
EPSILON = 1e-5


def setup_inputs(seed: int = 0, part: int = 0) -> dict:
    key_list = jax.random.split(jax.random.key(seed), 16)
    part_key = jax.random.fold_in(jax.random.key(seed + 1), part)
    in_scale = D_MODEL ** -0.5
    hidden = jax.random.normal(part_key, (BATCH_ROWS, SEQ_LEN, D_MODEL), jnp.float32)
    head_scale = jnp.exp(jax.random.uniform(key_list[0], (LAYERS, HEADS), jnp.float32, -1.2, 1.2))
    col_scale = jnp.repeat(head_scale, HEAD_DIM, axis=1)[:, None, :]
    dt_init = jnp.exp(jax.random.uniform(key_list[1], (LAYERS, HEADS), jnp.float32, math.log(0.001), math.log(0.1)))
    return {
        'hidden': hidden.astype(jnp.bfloat16),
        'norm_w': (1.0 + 0.2 * jax.random.normal(key_list[2], (LAYERS, D_MODEL), jnp.float32)).astype(jnp.bfloat16),
        'w_z': (in_scale * jax.random.normal(key_list[3], (LAYERS, D_MODEL, INNER_WIDTH), jnp.float32)).astype(jnp.bfloat16),
        'w_x': (in_scale * col_scale * jax.random.normal(key_list[4], (LAYERS, D_MODEL, INNER_WIDTH), jnp.float32)).astype(jnp.bfloat16),
        'w_bc': (in_scale * jax.random.normal(key_list[5], (LAYERS, D_MODEL, 2 * STATE_DIM), jnp.float32)).astype(jnp.bfloat16),
        'w_dt': (0.5 * in_scale * jax.random.normal(key_list[6], (LAYERS, D_MODEL, HEADS), jnp.float32)).astype(jnp.bfloat16),
        'conv_x': (0.5 * jax.random.normal(key_list[7], (LAYERS, CONV_WIDTH, INNER_WIDTH), jnp.float32)).astype(jnp.bfloat16),
        'conv_bc': (0.5 * jax.random.normal(key_list[8], (LAYERS, CONV_WIDTH, 2 * STATE_DIM), jnp.float32)).astype(jnp.bfloat16),
        'bias_x': (0.3 * jax.random.normal(key_list[9], (LAYERS, INNER_WIDTH), jnp.float32)).astype(jnp.bfloat16),
        'bias_bc': (0.3 * jax.random.normal(key_list[10], (LAYERS, 2 * STATE_DIM), jnp.float32)).astype(jnp.bfloat16),
        'dt_bias': dt_init + jnp.log(-jnp.expm1(-dt_init)),
        'a_log': jnp.log(jax.random.uniform(key_list[11], (LAYERS, HEADS), jnp.float32, 1.0, 16.0)),
        'd_skip': jax.random.uniform(key_list[12], (LAYERS, HEADS), jnp.float32, 0.5, 2.0),
        'gate_w': (1.0 + 0.2 * jax.random.normal(key_list[13], (LAYERS, INNER_WIDTH), jnp.float32)).astype(jnp.bfloat16),
        'w_out': (INNER_WIDTH ** -0.5 * jax.random.normal(key_list[14], (LAYERS, INNER_WIDTH, D_MODEL), jnp.float32)).astype(jnp.bfloat16),
    }


def causal_conv(seq_in, kernel, conv_bias):
    n_steps = seq_in.shape[1]
    padded = jnp.pad(seq_in, ((0, 0), (CONV_WIDTH - 1, 0), (0, 0)))
    conv_sum = conv_bias.astype(jnp.float32)
    for tap_index in range(CONV_WIDTH):
        conv_sum = conv_sum + padded[:, tap_index:tap_index + n_steps, :].astype(jnp.float32) * kernel[tap_index].astype(jnp.float32)
    return conv_sum


def ssd_sequence(seq_in):
    x_heads, dt_val, a_vals, b_in, c_in = seq_in
    n_blocks = SEQ_LEN // BLOCK_LEN
    step_ids = jnp.arange(BLOCK_LEN)
    lower_tri = step_ids[:, None] >= step_ids[None, :]

    def block_step(state, block):
        x_block, dt_block, a_block, b_block, c_block = block
        a_cum = jnp.cumsum(a_block, axis=0)
        seg_sum = a_cum[:, None, :] - a_cum[None, :, :]
        decay_mat = jnp.where(lower_tri[:, :, None], jnp.exp(jnp.minimum(seg_sum, 0.0)), 0.0)
        c_dot_b = jnp.einsum('in,jn->ij', c_block, b_block)
        x_dt = x_block * dt_block[:, :, None]
        y_in = jnp.einsum('ijh,jhp->ihp', decay_mat * c_dot_b[:, :, None], x_dt)
        y_st = jnp.einsum('in,hpn->ihp', c_block, state) * jnp.exp(a_cum)[:, :, None]
        tail_decay = jnp.exp(a_cum[-1][None, :] - a_cum)
        new_state = state * jnp.exp(a_cum[-1])[:, None, None] + jnp.einsum('jn,jhp->hpn', b_block, x_dt * tail_decay[:, :, None])
        return new_state, y_in + y_st

    blocks_in = (
        x_heads.reshape(n_blocks, BLOCK_LEN, HEADS, HEAD_DIM),
        dt_val.reshape(n_blocks, BLOCK_LEN, HEADS),
        a_vals.reshape(n_blocks, BLOCK_LEN, HEADS),
        b_in.reshape(n_blocks, BLOCK_LEN, STATE_DIM),
        c_in.reshape(n_blocks, BLOCK_LEN, STATE_DIM),
    )
    init_state = jnp.zeros((HEADS, HEAD_DIM, STATE_DIM), jnp.float32)
    last_state, y_blocks = lax.scan(block_step, init_state, blocks_in)
    return y_blocks.reshape(SEQ_LEN, HEADS, HEAD_DIM)


def mixer_layer(current, layer_params):
    norm_w, w_z, w_x, w_bc, w_dt, conv_x, conv_bc, bias_x, bias_bc, dt_bias, a_log, d_skip, gate_w, w_out = layer_params
    tokens = BATCH_ROWS * SEQ_LEN
    residual = current.astype(jnp.float32)
    normed = (residual * lax.rsqrt(jnp.mean(residual * residual, axis=-1, keepdims=True) + EPSILON) * norm_w.astype(jnp.float32)).astype(jnp.bfloat16)
    flat_in = normed.reshape(tokens, D_MODEL)
    gate_z = jnp.dot(flat_in, w_z, preferred_element_type=jnp.float32).astype(jnp.bfloat16)
    x_pre = jnp.dot(flat_in, w_x, preferred_element_type=jnp.float32).astype(jnp.bfloat16)
    bc_pre = jnp.dot(flat_in, w_bc, preferred_element_type=jnp.float32).astype(jnp.bfloat16)
    dt_pre = jnp.dot(flat_in, w_dt, preferred_element_type=jnp.float32).astype(jnp.bfloat16)
    x_act = jax.nn.silu(causal_conv(x_pre.reshape(BATCH_ROWS, SEQ_LEN, INNER_WIDTH), conv_x, bias_x))
    bc_act = jax.nn.silu(causal_conv(bc_pre.reshape(BATCH_ROWS, SEQ_LEN, 2 * STATE_DIM), conv_bc, bias_bc))
    dt_val = jax.nn.softplus(dt_pre.astype(jnp.float32).reshape(BATCH_ROWS, SEQ_LEN, HEADS) + dt_bias)
    a_vals = -dt_val * jnp.exp(a_log)
    x_heads = x_act.reshape(BATCH_ROWS, SEQ_LEN, HEADS, HEAD_DIM)
    y_heads = lax.map(ssd_sequence, (x_heads, dt_val, a_vals, bc_act[..., :STATE_DIM], bc_act[..., STATE_DIM:]))
    y_heads = y_heads + d_skip[:, None] * x_heads
    gated_v = y_heads.reshape(BATCH_ROWS, SEQ_LEN, INNER_WIDTH) * jax.nn.silu(gate_z.astype(jnp.float32).reshape(BATCH_ROWS, SEQ_LEN, INNER_WIDTH))
    normed_y = (gated_v * lax.rsqrt(jnp.mean(gated_v * gated_v, axis=-1, keepdims=True) + EPSILON) * gate_w.astype(jnp.float32)).astype(jnp.bfloat16)
    mixed_out = jnp.dot(normed_y.reshape(tokens, INNER_WIDTH), w_out, preferred_element_type=jnp.float32)
    return (residual + mixed_out.reshape(BATCH_ROWS, SEQ_LEN, D_MODEL)).astype(jnp.bfloat16)


def reference(hidden, norm_w, w_z, w_x, w_bc, w_dt, conv_x, conv_bc, bias_x, bias_bc, dt_bias, a_log, d_skip, gate_w, w_out):
    params = (norm_w, w_z, w_x, w_bc, w_dt, conv_x, conv_bc, bias_x, bias_bc, dt_bias, a_log, d_skip, gate_w, w_out)

    def layer_step(current, layer_params):
        return mixer_layer(current, layer_params), None

    final_hidden, unused = lax.scan(layer_step, hidden, params)
    return final_hidden
```

```python
import functools

import jax
import jax.numpy as jnp
from jax import lax
from jax.experimental import pallas as pl
from jax.experimental.pallas import tpu as pltpu
from jax.sharding import PartitionSpec as P

EPS = 1e-5
T = 128
HEAD = 64
STATE = 64
HI = lax.Precision.HIGHEST
F32 = jnp.float32
BF16 = jnp.bfloat16


def mixer_kernel(n_layers, n_chunks, inner_width,
                 hid_ref, norm_ref, wz_ref, wx_ref, wbc_ref, wdt_ref, convx_ref, convbc_ref, biasx_ref,
                 biasbc_ref, dtb_ref, alog_ref, dskip_ref, gate_ref, wout_ref,
                 out_ref,
                 w_in, w_o, wdt_s, hid_s, u_buf, p_buf, r0, r1a, r1b, r2a, r2b, h_buf, c_buf, zd_buf,
                 x_act, v_buf, s_buf, cs_buf, acum_s, acumt_s, dt_s, g_s, bt_s, stats,
                 norm_s, cw_s, cb_s, dtb_s, nega_s, dsk_s, gate_s,
                 w_sem, h_sem, o_sem, send_sem, recv_sem, st_send, st_recv):
    d_model = u_buf.shape[2]
    width = x_act.shape[1]
    n_pairs = width // (2 * HEAD)
    n_heads = dtb_ref.shape[1]
    conv_w = width + 2 * STATE
    n_items = n_layers * n_chunks

    me = lax.axis_index("tp")
    core = lax.rem(me, 2)
    xi = lax.rem(me // 2, 2)
    yi = me // 4

    def peer_id(dx, dy, dc):
        px = xi if dx == 0 else 1 - xi
        py = yi if dy == 0 else 1 - yi
        pc = core if dc == 0 else 1 - core
        return {"tp": py * 4 + px * 2 + pc}

    relations = [(dx, dy, dc) for dx in (0, 1) for dy in (0, 1) for dc in (0, 1)][1:]
    core_peer, x_peer, y_peer = peer_id(0, 0, 1), peer_id(1, 0, 0), peer_id(0, 1, 0)

    def weight_copies(l):
        return [
            pltpu.make_async_copy(wx_ref.at[l], w_in.at[l, :, pl.ds(0, width)], w_sem.at[l, 0]),
            pltpu.make_async_copy(wbc_ref.at[l], w_in.at[l, :, pl.ds(width, 2 * STATE)], w_sem.at[l, 1]),
            pltpu.make_async_copy(wz_ref.at[l], w_in.at[l, :, pl.ds(conv_w + 128, width)], w_sem.at[l, 2]),
            pltpu.make_async_copy(wdt_ref.at[l], wdt_s.at[l], w_sem.at[l, 3]),
        ]

    def out_weight_copy(l):
        return pltpu.make_async_copy(wout_ref.at[l], w_o.at[l], w_sem.at[l, 4])

    def hid_copy(c):
        rows = pl.ds(c * T, T)
        return pltpu.make_async_copy(hid_ref.at[0, rows, :], hid_s.at[rows, :], h_sem.at[c])

    def out_copy(c):
        rows = pl.ds(c * T, T)
        return pltpu.make_async_copy(hid_s.at[rows, :], out_ref.at[0, rows, :], o_sem.at[c])

    hid_copy(0).start()
    for cp in weight_copies(0):
        cp.start()
    out_weight_copy(0).start()
    for c in range(1, n_chunks):
        hid_copy(c).start()
    for l in range(1, n_layers):
        for cp in weight_copies(l):
            cp.start()
        out_weight_copy(l).start()

    barrier = pltpu.get_barrier_semaphore()
    for rel in relations:
        pl.semaphore_signal(barrier, inc=1, device_id=peer_id(*rel))

    lane = lax.broadcasted_iota(jnp.int32, (1, 128), 1)
    for l in range(n_layers):
        norm_s[l] = norm_ref[l:l + 1, :].astype(F32)
        cw_s[l, :, 0:width] = convx_ref[l].astype(F32)
        cw_s[l, :, width:conv_w] = convbc_ref[l].astype(F32)
        cb_s[l, :, 0:width] = biasx_ref[l:l + 1, :].astype(F32)
        cb_s[l, :, width:conv_w] = biasbc_ref[l:l + 1, :].astype(F32)
        gate_s[l] = gate_ref[l:l + 1, :].astype(F32)
        dtb_s[l] = jnp.zeros((1, 128), F32)
        nega_s[l] = jnp.zeros((1, 128), F32)
        dtb_s[l, :, 0:n_heads] = dtb_ref[l:l + 1, :]
        nega_s[l, :, 0:n_heads] = -jnp.exp(alog_ref[l:l + 1, :])
        for p in range(n_pairs):
            d0 = dskip_ref[l:l + 1, 2 * p:2 * p + 1]
            d1 = dskip_ref[l:l + 1, 2 * p + 1:2 * p + 2]
            dsk_s[l, :, 128 * p:128 * (p + 1)] = jnp.where(lane < HEAD, d0, d1)

    def rdma(kind, j):
        l, c = j // n_chunks, lax.rem(j, n_chunks)
        base = pl.multiple_of(c * T, T)
        mine = pl.multiple_of(core * (T // 2), T // 2)
        theirs = pl.multiple_of((1 - core) * (T // 2), T // 2)
        if kind == 0:
            src, dst, dev = p_buf.at[lax.rem(j, 2), pl.ds(theirs, T // 2), :], r0.at[j], core_peer
        elif kind == 1:
            src, dst, dev = r0.at[j, pl.ds(pl.multiple_of((1 - xi) * 16, 16), 16), :], r1a.at[j], x_peer
        elif kind == 2:
            src, dst, dev = r0.at[j, pl.ds(pl.multiple_of(32 + (1 - yi) * 16, 16), 16), :], r1b.at[j], y_peer
        elif kind == 3:
            src, dst, dev = r1a.at[j, pl.ds(pl.multiple_of((1 - yi) * 8, 8), 8), :], r2a.at[j], y_peer
        elif kind == 4:
            src, dst, dev = r1b.at[j, pl.ds(pl.multiple_of((1 - xi) * 8, 8), 8), :], r2b.at[j], x_peer
        else:
            if kind == 5:
                off, size, dev = base + mine + xi * 16 + yi * 8, 8, y_peer
            elif kind == 6:
                off, size, dev = base + mine + 32 + yi * 16 + xi * 8, 8, x_peer
            elif kind == 7:
                off, size, dev = base + mine + xi * 16, 16, x_peer
            elif kind == 8:
                off, size, dev = base + mine + 32 + yi * 16, 16, y_peer
            else:
                off, size, dev = base + mine, T // 2, core_peer
            src = u_buf.at[l + 1, pl.ds(pl.multiple_of(off, 8), size), :]
            dst = src
        return pltpu.make_async_remote_copy(
            src_ref=src, dst_ref=dst, send_sem=send_sem.at[j, kind], recv_sem=recv_sem.at[j, kind],
            device_id=dev, device_id_type=pl.DeviceIdType.MESH)

    def stat_copy(r, j):
        return pltpu.make_async_remote_copy(
            src_ref=stats.at[j, pl.ds(0, 1), :], dst_ref=stats.at[j, pl.ds(r + 1, 1), :],
            send_sem=st_send.at[j, r], recv_sem=st_recv.at[j, r],
            device_id=peer_id(*relations[r]), device_id_type=pl.DeviceIdType.MESH)

    def in_proj(j):
        l, c = j // n_chunks, lax.rem(j, n_chunks)
        base = pl.multiple_of(c * T, T)

        @pl.when(l == 0)
        def _():
            hid_copy(c).wait()

            @pl.loop(0, T // 16)
            def _(i):
                rows = pl.ds(pl.multiple_of(base + i * 16, 16), 16)
                u_buf[0, rows, :] = hid_s[rows, :].astype(F32)

        @pl.loop(0, T // 16)
        def _(i):
            u = u_buf[l, pl.ds(pl.multiple_of(base + i * 16, 16), 16), :]
            ms = jnp.mean(u * u, axis=-1, keepdims=True)
            h = u * lax.rsqrt(ms + EPS) * norm_s[l]
            h_buf[pl.ds(pl.multiple_of(i * 16, 16), 16), :] = h.astype(BF16)

        @pl.when(c == 0)
        def _():
            for cp in weight_copies(l):
                cp.wait()

            @pl.loop(0, d_model // 256)
            def _(i):
                rows = pl.ds(pl.multiple_of(i * 256, 256), 256)
                w_in[l, rows, conv_w:conv_w + 128] = jnp.zeros((256, 128), BF16)
                w_in[l, rows, conv_w:conv_w + n_heads] = wdt_s[l, rows, :]

            c_buf[0:8, :] = jnp.zeros((8, conv_w), F32)
            s_buf[...] = jnp.zeros_like(s_buf)

        @pl.when(c > 0)
        def _():
            c_buf[0:8, :] = c_buf[T:T + 8, :]

        h = h_buf[...]
        for n in range(0, conv_w, 256):
            r = jnp.dot(h, w_in[l, :, n:n + 256], preferred_element_type=F32)
            c_buf[8:8 + T, n:n + 256] = r.astype(BF16).astype(F32)
        for n in range(0, width + 128, 256):
            r = jnp.dot(h, w_in[l, :, conv_w + n:conv_w + n + 256], preferred_element_type=F32)
            zd_buf[:, n:n + 256] = r.astype(BF16).astype(F32)

    def scan_prep(j):
        l = j // n_chunks
        b_act = None
        for n in range(0, conv_w, 128):
            cols = slice(n, n + 128)
            acc = cb_s[l, :, cols] + c_buf[5:5 + T, cols] * cw_s[l, 0:1, cols]
            for k in range(1, 4):
                acc = acc + c_buf[5 + k:5 + k + T, cols] * cw_s[l, k:k + 1, cols]
            act = acc * jax.nn.sigmoid(acc)
            if n < width:
                x_act[:, cols] = act
            else:
                b_act = act
        bt = b_act.T
        c_mat = b_act[:, STATE:2 * STATE]
        bt_s[...] = bt[0:STATE, :]
        g_s[...] = jnp.dot(c_mat, bt[0:STATE, :], precision=HI, preferred_element_type=F32)
        cs_buf[...] = jnp.dot(c_mat, s_buf[...], precision=HI, preferred_element_type=F32)
        dt = jax.nn.softplus(zd_buf[:, 0:128] + dtb_s[l])
        a = dt * nega_s[l]
        row = lax.broadcasted_iota(jnp.int32, (T, T), 0)
        col = lax.broadcasted_iota(jnp.int32, (T, T), 1)
        tril = jnp.where(row >= col, 1.0, 0.0).astype(F32)
        acum = jnp.dot(tril, a, precision=HI, preferred_element_type=F32)
        dt_s[...] = dt
        acum_s[...] = acum
        acumt_s[...] = acum.T

    def scan_heads(j):
        l = j // n_chunks
        slot = lax.rem(j, 2)
        row = lax.broadcasted_iota(jnp.int32, (T, T), 0)
        col = lax.broadcasted_iota(jnp.int32, (T, T), 1)
        causal = row >= col
        low = col < HEAD
        low_row = lane < HEAD
        g = g_s[...]
        bt = bt_s[...]
        sq = jnp.zeros((T, 128), F32)
        for p in range(n_pairs):
            h0, h1 = 2 * p, 2 * p + 1
            cols = slice(128 * p, 128 * (p + 1))
            a0 = jnp.broadcast_to(acum_s[:, h0:h0 + 1], (T, T))
            a1 = jnp.broadcast_to(acum_s[:, h1:h1 + 1], (T, T))
            m0 = jnp.where(causal, jnp.exp(jnp.minimum(a0 - acumt_s[h0:h0 + 1, :], 0.0)), 0.0) * g
            m1 = jnp.where(causal, jnp.exp(jnp.minimum(a1 - acumt_s[h1:h1 + 1, :], 0.0)), 0.0) * g
            dt = jnp.where(low, dt_s[:, h0:h0 + 1], dt_s[:, h1:h1 + 1])
            x = x_act[:, cols]
            xd = x * dt
            both = jnp.concatenate([m0, m1], axis=1)
            split = jnp.concatenate([jnp.where(low, xd, 0.0), jnp.where(low, 0.0, xd)], axis=0)
            y = jnp.dot(both, split, precision=HI, preferred_element_type=F32)
            ap = jnp.where(low, a0, a1)
            last = jnp.where(low_row, acum_s[T - 1:T, h0:h0 + 1], acum_s[T - 1:T, h1:h1 + 1])
            y = y + cs_buf[:, cols] * jnp.exp(ap)
            xt = xd * jnp.exp(last - ap)
            s_buf[:, cols] = s_buf[:, cols] * jnp.exp(last) + jnp.dot(bt, xt, precision=HI, preferred_element_type=F32)
            y = y + dsk_s[l, :, cols] * x
            z = zd_buf[:, 128 + 128 * p:256 + 128 * p]
            v = y * (z * jax.nn.sigmoid(z))
            v_buf[slot, :, cols] = v
            sq = sq + v * v
        ones = jnp.ones((8, 128), F32)
        part = lax.dot_general(ones, sq, (((1,), (1,)), ((), ())), precision=HI, preferred_element_type=F32)
        stats[j, 0:1, :] = part[0:1, :]
        for r in range(len(relations)):
            stat_copy(r, j).start()

    def out_proj(j):
        l, c = j // n_chunks, lax.rem(j, n_chunks)
        slot = lax.rem(j, 2)

        @pl.when(c == 0)
        def _():
            out_weight_copy(l).wait()

        for r in range(len(relations)):
            stat_copy(r, j).wait()
        total = jnp.sum(stats[j], axis=0, keepdims=True)
        rs = lax.rsqrt(total * (1.0 / inner_width) + EPS)
        rs_t = jnp.broadcast_to(rs, (T, T)).T
        parts = []
        for p in range(n_pairs):
            cols = slice(128 * p, 128 * (p + 1))
            parts.append((v_buf[slot, :, cols] * rs_t * gate_s[l, :, cols]).astype(BF16))
        g = jnp.concatenate(parts, axis=1)
        for n in range(0, d_model, 256):
            p_buf[slot, :, n:n + 256] = jnp.dot(g, w_o[l, :, n:n + 256], preferred_element_type=F32)
        rdma(0, j).start()

    def ev1(j):
        slot = lax.rem(j, 2)
        mine = core * (T // 2)
        rdma(0, j).wait()

        def add(off):
            off = pl.multiple_of(off, 16)
            r0[j, pl.ds(off, 16), :] += p_buf[slot, pl.ds(pl.multiple_of(mine + off, 16), 16), :]

        add((1 - xi) * 16)
        rdma(1, j).start()
        add(32 + (1 - yi) * 16)
        rdma(2, j).start()
        add(xi * 16)
        add(32 + yi * 16)

    def ev2(j):
        rdma(1, j).wait()
        r1a[j] += r0[j, pl.ds(pl.multiple_of(xi * 16, 16), 16), :]
        rdma(3, j).start()
        rdma(2, j).wait()
        r1b[j] += r0[j, pl.ds(pl.multiple_of(32 + yi * 16, 16), 16), :]
        rdma(4, j).start()

    def ev3(j):
        l, c = j // n_chunks, lax.rem(j, n_chunks)
        base = c * T + core * (T // 2)
        rows_a = pl.ds(pl.multiple_of(base + xi * 16 + yi * 8, 8), 8)
        rows_b = pl.ds(pl.multiple_of(base + 32 + yi * 16 + xi * 8, 8), 8)
        rdma(3, j).wait()
        val = r2a[j] + r1a[j, pl.ds(pl.multiple_of(yi * 8, 8), 8), :]
        u_buf[l + 1, rows_a, :] = (u_buf[l, rows_a, :] + val).astype(BF16).astype(F32)
        rdma(5, j).start()
        rdma(4, j).wait()
        val = r2b[j] + r1b[j, pl.ds(pl.multiple_of(xi * 8, 8), 8), :]
        u_buf[l + 1, rows_b, :] = (u_buf[l, rows_b, :] + val).astype(BF16).astype(F32)
        rdma(6, j).start()

    def ev4(j):
        rdma(5, j).wait()
        rdma(7, j).start()
        rdma(6, j).wait()
        rdma(8, j).start()

    def ev5(j):
        rdma(7, j).wait()
        rdma(8, j).wait()
        rdma(9, j).start()

    def ev6(j):
        l, c = j // n_chunks, lax.rem(j, n_chunks)
        rdma(9, j).wait()

        @pl.when(l == n_layers - 1)
        def _():
            @pl.loop(0, T // 16)
            def _(i):
                rows = pl.ds(pl.multiple_of(c * T + i * 16, 16), 16)
                hid_s[rows, :] = u_buf[n_layers, rows, :].astype(BF16)

            out_copy(c).start()

    def guarded(stage, j):
        pl.when(jnp.logical_and(j >= 0, j < n_items))(lambda: stage(j))

    pl.semaphore_wait(barrier, len(relations))

    @pl.loop(0, n_items + 3)
    def _(j):
        guarded(in_proj, j)
        guarded(ev2, j - 2)
        guarded(ev4, j - 3)
        guarded(out_proj, j - 1)
        guarded(scan_prep, j)
        guarded(ev1, j - 1)
        guarded(scan_heads, j)
        guarded(ev3, j - 2)
        guarded(ev5, j - 3)
        guarded(ev6, j - 3)

    for c in range(n_chunks):
        out_copy(c).wait()


def solution(mesh):
    tp_size = mesh.shape['tp']
    rep_spec = P()
    col_spec = P(None, None, 'tp')
    vec_spec = P(None, 'tp')
    in_specs = (P('dp'), rep_spec, col_spec, col_spec, rep_spec, col_spec, col_spec, rep_spec, vec_spec, rep_spec,
                vec_spec, vec_spec, vec_spec, vec_spec, P(None, 'tp', None))

    def device_forward(hidden, norm_w, w_z, w_x, w_bc, w_dt, conv_x, conv_bc, bias_x, bias_bc, dt_bias, a_log,
                       d_skip, gate_w, w_out):
        n_layers, d_model = norm_w.shape
        n_tok = hidden.shape[1]
        width = w_x.shape[-1]
        n_heads = dt_bias.shape[-1]
        conv_w = width + 2 * STATE
        n_chunks = n_tok // T
        n_items = n_layers * n_chunks
        any_spec = pl.BlockSpec(memory_space=pl.ANY)
        vmem_spec = pl.BlockSpec(memory_space=pltpu.VMEM)
        dma = pltpu.SemaphoreType.DMA
        return pl.pallas_call(
            functools.partial(mixer_kernel, n_layers, n_chunks, width * tp_size),
            out_shape=jax.ShapeDtypeStruct(hidden.shape, BF16),
            in_specs=[any_spec, vmem_spec, any_spec, any_spec, any_spec, any_spec] + [vmem_spec] * 8 + [any_spec],
            out_specs=any_spec,
            scratch_shapes=[
                pltpu.VMEM((n_layers, d_model, conv_w + 128 + width), BF16),
                pltpu.VMEM((n_layers, width, d_model), BF16),
                pltpu.VMEM((n_layers, d_model, n_heads), BF16),
                pltpu.VMEM((n_tok, d_model), BF16),
                pltpu.VMEM((n_layers + 1, n_tok, d_model), F32),
                pltpu.VMEM((2, T, d_model), F32),
                pltpu.VMEM((n_items, T // 2, d_model), F32),
                pltpu.VMEM((n_items, T // 8, d_model), F32),
                pltpu.VMEM((n_items, T // 8, d_model), F32),
                pltpu.VMEM((n_items, T // 16, d_model), F32),
                pltpu.VMEM((n_items, T // 16, d_model), F32),
                pltpu.VMEM((T, d_model), BF16),
                pltpu.VMEM((T + 8, conv_w), F32),
                pltpu.VMEM((T, 128 + width), F32),
                pltpu.VMEM((T, width), F32),
                pltpu.VMEM((2, T, width), F32),
                pltpu.VMEM((STATE, width), F32),
                pltpu.VMEM((T, width), F32),
                pltpu.VMEM((T, 128), F32),
                pltpu.VMEM((128, T), F32),
                pltpu.VMEM((T, 128), F32),
                pltpu.VMEM((T, T), F32),
                pltpu.VMEM((STATE, T), F32),
                pltpu.VMEM((n_items, 8, T), F32),
                pltpu.VMEM((n_layers, 1, d_model), F32),
                pltpu.VMEM((n_layers, 4, conv_w), F32),
                pltpu.VMEM((n_layers, 1, conv_w), F32),
                pltpu.VMEM((n_layers, 1, 128), F32),
                pltpu.VMEM((n_layers, 1, 128), F32),
                pltpu.VMEM((n_layers, 1, width), F32),
                pltpu.VMEM((n_layers, 1, width), F32),
                dma((n_layers, 5)),
                dma((n_chunks,)),
                dma((n_chunks,)),
                dma((n_items, 10)),
                dma((n_items, 10)),
                dma((n_items, 7)),
                dma((n_items, 7)),
            ],
            compiler_params=pltpu.CompilerParams(
                collective_id=0, has_side_effects=True, vmem_limit_bytes=67043328),
            name="mixer",
        )(hidden, norm_w, w_z, w_x, w_bc, w_dt, conv_x, conv_bc, bias_x, bias_bc, dt_bias, a_log, d_skip, gate_w,
          w_out)

    return jax.shard_map(device_forward, mesh=mesh, in_specs=in_specs, out_specs=P('dp'), check_vma=False)
```

```python
import functools

import jax
import jax.numpy as jnp
from jax import lax
from jax.experimental import pallas as pl
from jax.experimental.pallas import tpu as pltpu
from jax.sharding import PartitionSpec as P

EPS = 1e-5
T = 128
HEAD = 64
STATE = 64
HI = lax.Precision.HIGHEST
F32 = jnp.float32
BF16 = jnp.bfloat16


def mixer_kernel(n_layers, n_chunks, inner_width,
                 hid_ref, norm_ref, wz_ref, wx_ref, wbc_ref, wdt_ref, convx_ref, convbc_ref, biasx_ref,
                 biasbc_ref, dtb_ref, alog_ref, dskip_ref, gate_ref, wout_ref,
                 out_ref,
                 w_in, w_o, wdt_s, wdt_f, hid_s, u_buf, p_buf, r0, r1a, r1b, r2a, r2b, h_buf, c_buf, zd_buf,
                 x_act, v_buf, g_buf, s_buf, cs_buf, acum_s, acumt_s, dt_s, g_s, bt_s, sq_s, f_s, stats,
                 norm_s, cw_s, cb_s, dtb_s, nega_s, dsk_s, gate_s,
                 w_sem, h_sem, o_sem, send_sem, recv_sem, st_send, st_recv):
    d_model = u_buf.shape[2]
    half = d_model // 2
    width = x_act.shape[1]
    n_pairs = width // (2 * HEAD)
    n_heads = dtb_ref.shape[1]
    conv_w = width + 2 * STATE
    n_items = n_layers * n_chunks

    me = lax.axis_index("tp")
    core = lax.rem(me, 2)
    xi = lax.rem(me // 2, 2)
    yi = me // 4

    def peer_id(dx, dy, dc):
        px = xi if dx == 0 else 1 - xi
        py = yi if dy == 0 else 1 - yi
        pc = core if dc == 0 else 1 - core
        return {"tp": py * 4 + px * 2 + pc}

    relations = [(dx, dy, dc) for dx in (0, 1) for dy in (0, 1) for dc in (0, 1)][1:]
    core_peer, x_peer, y_peer = peer_id(0, 0, 1), peer_id(1, 0, 0), peer_id(0, 1, 0)

    def split_item(j):
        if isinstance(j, int):
            return j // n_chunks, j % n_chunks
        return j // n_chunks, lax.rem(j, n_chunks)

    halves = [slice(0, half), slice(half, d_model)]

    def at(off, size, unit=8):
        return pl.ds(pl.multiple_of(off, unit), size)

    def conv_weight_copies(l):
        return [
            pltpu.make_async_copy(wx_ref.at[l], w_in.at[l, :, pl.ds(0, width)], w_sem.at[l, 0]),
            pltpu.make_async_copy(wbc_ref.at[l], w_in.at[l, :, pl.ds(width, 2 * STATE)], w_sem.at[l, 0]),
        ]

    def gate_weight_copy(l):
        return pltpu.make_async_copy(wz_ref.at[l], w_in.at[l, :, pl.ds(conv_w + 128, width)], w_sem.at[l, 1])

    def out_weight_copy(l):
        return pltpu.make_async_copy(wout_ref.at[l], w_o.at[l], w_sem.at[l, 2])

    def dt_weight_copy():
        return pltpu.make_async_copy(wdt_ref, wdt_s, h_sem.at[2])

    def hid_copy(k):
        rows = pl.ds(0, T) if k == 0 else pl.ds(T, (n_chunks - 1) * T)
        return pltpu.make_async_copy(hid_ref.at[0, rows, :], hid_s.at[rows, :], h_sem.at[k])

    def out_copy(c, h):
        rows, cols = at(c * T, T, T), pl.ds(h * half, half)
        return pltpu.make_async_copy(hid_s.at[rows, cols], out_ref.at[0, rows, cols], o_sem)

    def start_in_weights(l):
        for cp in conv_weight_copies(l):
            cp.start()
        gate_weight_copy(l).start()

    hid_copy(0).start()
    dt_weight_copy().start()
    start_in_weights(0)

    barrier = pltpu.get_barrier_semaphore()
    for rel in relations:
        pl.semaphore_signal(barrier, inc=1, device_id=peer_id(*rel))

    lane = lax.broadcasted_iota(jnp.int32, (1, 128), 1)
    for l in range(n_layers):
        norm_s[l] = norm_ref[l:l + 1, :].astype(F32)
        cw_s[l, :, 0:width] = convx_ref[l].astype(F32)
        cw_s[l, :, width:conv_w] = convbc_ref[l].astype(F32)
        cb_s[l, :, 0:width] = biasx_ref[l:l + 1, :].astype(F32)
        cb_s[l, :, width:conv_w] = biasbc_ref[l:l + 1, :].astype(F32)
        gate_s[l] = gate_ref[l:l + 1, :].astype(F32)
        dtb_s[l] = jnp.zeros((1, 128), F32)
        nega_s[l] = jnp.zeros((1, 128), F32)
        dtb_s[l, :, 0:n_heads] = dtb_ref[l:l + 1, :]
        nega_s[l, :, 0:n_heads] = -jnp.exp(alog_ref[l:l + 1, :])
        for p in range(n_pairs):
            d0 = dskip_ref[l:l + 1, 2 * p:2 * p + 1]
            d1 = dskip_ref[l:l + 1, 2 * p + 1:2 * p + 2]
            dsk_s[l, :, 128 * p:128 * (p + 1)] = jnp.where(lane < HEAD, d0, d1)

    def rdma(kind, j, h):
        l, c = split_item(j)
        cols = pl.ds(h * half, half)
        mine = core * (T // 2)
        base = c * T + mine
        group = (kind + 1) // 2
        if kind == 0:
            src, dst, dev = p_buf.at[at((1 - core) * (T // 2), T // 2), cols], r0.at[j, :, cols], core_peer
        elif kind == 1:
            src, dst, dev = r0.at[j, at((1 - xi) * 16, 16), cols], r1a.at[j, :, cols], x_peer
        elif kind == 2:
            src, dst, dev = r0.at[j, at(32 + (1 - yi) * 16, 16), cols], r1b.at[j, :, cols], y_peer
        elif kind == 3:
            src, dst, dev = r1a.at[j, at((1 - yi) * 8, 8), cols], r2a.at[j, :, cols], y_peer
        elif kind == 4:
            src, dst, dev = r1b.at[j, at((1 - xi) * 8, 8), cols], r2b.at[j, :, cols], x_peer
        else:
            off, size, dev = [
                (base + xi * 16 + yi * 8, 8, y_peer),
                (base + 32 + yi * 16 + xi * 8, 8, x_peer),
                (base + xi * 16, 16, x_peer),
                (base + 32 + yi * 16, 16, y_peer),
                (base, T // 2, core_peer),
            ][kind - 5]
            src = u_buf.at[l + 1, at(off, size), cols]
            dst = src
        return pltpu.make_async_remote_copy(
            src_ref=src, dst_ref=dst, send_sem=send_sem.at[c, h, group], recv_sem=recv_sem.at[c, h, group],
            device_id=dev, device_id_type=pl.DeviceIdType.MESH)

    def wait_pair(kind, j, h):
        _, c = split_item(j)
        group = (kind + 1) // 2
        size = 32 if kind in (1, 7) else 16
        both = r0.at[j, pl.ds(0, size), pl.ds(h * half, half)]
        pltpu.make_async_copy(both, both, send_sem.at[c, h, group]).wait()
        pltpu.make_async_copy(both, both, recv_sem.at[c, h, group]).wait()

    def stat_copy(r, j):
        _, c = split_item(j)
        return pltpu.make_async_remote_copy(
            src_ref=stats.at[j, pl.ds(0, 1), :], dst_ref=stats.at[j, pl.ds(r + 1, 1), :],
            send_sem=st_send.at[c], recv_sem=st_recv.at[c],
            device_id=peer_id(*relations[r]), device_id_type=pl.DeviceIdType.MESH)

    def wait_stats(j):
        _, c = split_item(j)
        rows = stats.at[j, pl.ds(1, len(relations)), :]
        pltpu.make_async_copy(rows, rows, st_send.at[c]).wait()
        pltpu.make_async_copy(rows, rows, st_recv.at[c]).wait()

    def in_norm(j):
        l, c = split_item(j)
        base = c * T

        @pl.when(j == 0)
        def _():
            hid_copy(0).wait()

        @pl.when(j == 1)
        def _():
            hid_copy(1).wait()
            for k in range(1, n_layers):
                start_in_weights(k)
                out_weight_copy(k).start()

        @pl.when(l == 0)
        def _():
            @pl.loop(0, T // 16)
            def _(i):
                rows = at(base + i * 16, 16, 16)
                u_buf[0, rows, :] = hid_s[rows, :].astype(F32)

        @pl.loop(0, T // 16)
        def _(i):
            u = u_buf[l, at(base + i * 16, 16, 16), :]
            ms = jnp.mean(u * u, axis=-1, keepdims=True)
            h = u * lax.rsqrt(ms + EPS) * norm_s[l]
            h_buf[at(i * 16, 16, 16), :] = h.astype(BF16)

        @pl.when(c == 0)
        def _():
            c_buf[0:8, :] = jnp.zeros((8, conv_w), F32)
            s_buf[...] = jnp.zeros_like(s_buf)

        @pl.when(c > 0)
        def _():
            c_buf[0:8, :] = c_buf[T:T + 8, :]

    def in_conv(j):
        l, c = split_item(j)

        @pl.when(j == 0)
        def _():
            dt_weight_copy().wait()
            for k in range(n_layers):
                wdt_f[16 * k + 8:16 * k + 16, :] = jnp.zeros((8, d_model), F32)
            for n in range(n_heads):
                rows = wdt_s[n].astype(F32)
                for k in range(n_layers):
                    wdt_f[16 * k + n:16 * k + n + 1, :] = rows[k:k + 1, :]

        @pl.when(c == 0)
        def _():
            w_in[l, :, conv_w:conv_w + 128] = jnp.zeros((d_model, 128), BF16)
            w_in[l, :, conv_w:conv_w + 16] = wdt_f[at(16 * l, 16), :].T.astype(BF16)
            both = w_in.at[l, :, pl.ds(0, conv_w)]
            pltpu.make_async_copy(both, both, w_sem.at[l, 0]).wait()

        h = h_buf[...]
        for n in range(0, conv_w, 256):
            r = jnp.dot(h, w_in[l, :, n:n + 256], preferred_element_type=F32)
            c_buf[8:8 + T, n:n + 256] = r.astype(BF16).astype(F32)

    def in_gate(j):
        l, c = split_item(j)

        @pl.when(c == 0)
        def _():
            gate_weight_copy(l).wait()

        @pl.when(j == 0)
        def _():
            out_weight_copy(0).start()
            hid_copy(1).start()

        h = h_buf[...]
        for n in range(0, width + 128, 256):
            r = jnp.dot(h, w_in[l, :, conv_w + n:conv_w + n + 256], preferred_element_type=F32)
            zd_buf[:, n:n + 256] = r.astype(BF16).astype(F32)

    def scan_prep(j):
        l, _ = split_item(j)
        b_act = None
        for n in range(0, conv_w, 128):
            cols = slice(n, n + 128)
            acc = cb_s[l, :, cols] + c_buf[5:5 + T, cols] * cw_s[l, 0:1, cols]
            for k in range(1, 4):
                acc = acc + c_buf[5 + k:5 + k + T, cols] * cw_s[l, k:k + 1, cols]
            act = acc * jax.nn.sigmoid(acc)
            if n < width:
                x_act[:, cols] = act
            else:
                b_act = act
        bt = b_act.T[0:STATE, :]
        c_mat = b_act[:, STATE:2 * STATE]
        bt_s[...] = bt
        g_s[...] = jnp.dot(c_mat, bt, precision=HI, preferred_element_type=F32)
        cs_buf[...] = jnp.dot(c_mat, s_buf[...], precision=HI, preferred_element_type=F32)
        dt = jax.nn.softplus(zd_buf[:, 0:128] + dtb_s[l])
        a = dt * nega_s[l]
        row = lax.broadcasted_iota(jnp.int32, (T, T), 0)
        col = lax.broadcasted_iota(jnp.int32, (T, T), 1)
        tril = jnp.where(row >= col, 1.0, 0.0).astype(F32)
        acum = jnp.dot(tril, a, precision=HI, preferred_element_type=F32)
        dt_s[...] = dt
        acum_s[...] = acum
        acumt_s[...] = acum.T

    def scan_pairs(j, pairs):
        l, _ = split_item(j)
        row = lax.broadcasted_iota(jnp.int32, (T, T), 0)
        col = lax.broadcasted_iota(jnp.int32, (T, T), 1)
        causal = row >= col
        low = col < HEAD
        low_row = lane < HEAD
        g = g_s[...]
        bt = bt_s[...]
        sq = jnp.zeros((T, 128), F32)
        for p in pairs:
            h0, h1 = 2 * p, 2 * p + 1
            cols = slice(128 * p, 128 * (p + 1))
            a0 = jnp.broadcast_to(acum_s[:, h0:h0 + 1], (T, T))
            a1 = jnp.broadcast_to(acum_s[:, h1:h1 + 1], (T, T))
            m0 = jnp.where(causal, jnp.exp(jnp.minimum(a0 - acumt_s[h0:h0 + 1, :], 0.0)), 0.0) * g
            m1 = jnp.where(causal, jnp.exp(jnp.minimum(a1 - acumt_s[h1:h1 + 1, :], 0.0)), 0.0) * g
            dt = jnp.where(low, dt_s[:, h0:h0 + 1], dt_s[:, h1:h1 + 1])
            x = x_act[:, cols]
            xd = x * dt
            both = jnp.concatenate([m0, m1], axis=1)
            split = jnp.concatenate([jnp.where(low, xd, 0.0), jnp.where(low, 0.0, xd)], axis=0)
            y = jnp.dot(both, split, precision=HI, preferred_element_type=F32)
            ap = jnp.where(low, a0, a1)
            last = jnp.where(low_row, acum_s[T - 1:T, h0:h0 + 1], acum_s[T - 1:T, h1:h1 + 1])
            y = y + cs_buf[:, cols] * jnp.exp(ap)
            xt = xd * jnp.exp(last - ap)
            s_buf[:, cols] = s_buf[:, cols] * jnp.exp(last) + jnp.dot(bt, xt, precision=HI, preferred_element_type=F32)
            y = y + dsk_s[l, :, cols] * x
            z = zd_buf[:, 128 + 128 * p:256 + 128 * p]
            v = y * (z * jax.nn.sigmoid(z))
            v_buf[:, cols] = v
            sq = sq + v * v
        return sq

    first_pairs = (n_pairs + 1) // 2

    def scan_a(j):
        sq_s[...] = scan_pairs(j, range(first_pairs))

    def scan_b(j):
        l, _ = split_item(j)
        sq = sq_s[...] + scan_pairs(j, range(first_pairs, n_pairs))
        ones = jnp.ones((8, 128), F32)
        part = lax.dot_general(ones, sq, (((1,), (1,)), ((), ())), precision=HI, preferred_element_type=F32)
        stats[j, 0:1, :] = part[0:1, :]
        for r in range(len(relations)):
            stat_copy(r, j).start()
        own = lax.rsqrt(jnp.sum(sq, axis=1, keepdims=True) * (1.0 / width) + EPS)
        for p in range(n_pairs):
            cols = slice(128 * p, 128 * (p + 1))
            g_buf[:, cols] = (v_buf[:, cols] * own * gate_s[l, :, cols]).astype(BF16)

    def out_proj(j, h):
        l, c = split_item(j)
        if h == 0:
            @pl.when(c == 0)
            def _():
                out_weight_copy(l).wait()

        g = g_buf[...]
        for n in range(h * half, (h + 1) * half, 256):
            p_buf[:, n:n + 256] = jnp.dot(g, w_o[l, :, n:n + 256], preferred_element_type=F32)
        rdma(0, j, h).start()

    def factors(j):
        wait_stats(j)
        st = stats[j]
        rs = lax.rsqrt(jnp.sum(st, axis=0, keepdims=True) * (1.0 / inner_width) + EPS)
        for k in range(2):
            own = lax.rsqrt(st[k:k + 1, :] * (1.0 / width) + EPS)
            f = rs / jnp.maximum(own, 1e-30)
            f_s[k] = jnp.broadcast_to(f, (T, T)).T

    def ev1(j, h):
        if h == 1:
            factors(j)
        mine = core * (T // 2)
        rdma(0, j, h).wait()

        def add(off):
            f_me = f_s[0, at(mine + off, 16), :]
            f_peer = f_s[1, at(mine + off, 16), :]
            for n in range(h * half, (h + 1) * half, 128):
                cols = slice(n, n + 128)
                r0[j, at(off, 16), cols] = r0[j, at(off, 16), cols] * f_peer + p_buf[at(mine + off, 16), cols] * f_me

        add((1 - xi) * 16)
        rdma(1, j, h).start()
        add(32 + (1 - yi) * 16)
        rdma(2, j, h).start()
        add(xi * 16)
        add(32 + yi * 16)

    def ev2(j, h):
        cols = halves[h]
        wait_pair(1, j, h)
        r1a[j, :, cols] += r0[j, at(xi * 16, 16), cols]
        rdma(3, j, h).start()
        r1b[j, :, cols] += r0[j, at(32 + yi * 16, 16), cols]
        rdma(4, j, h).start()

    def ev3(j, h):
        l, c = split_item(j)
        cols = halves[h]
        base = c * T + core * (T // 2)
        rows_a = at(base + xi * 16 + yi * 8, 8)
        rows_b = at(base + 32 + yi * 16 + xi * 8, 8)
        wait_pair(3, j, h)
        val = r2a[j, :, cols] + r1a[j, at(yi * 8, 8), cols]
        u_buf[l + 1, rows_a, cols] = (u_buf[l, rows_a, cols] + val).astype(BF16).astype(F32)
        rdma(5, j, h).start()
        val = r2b[j, :, cols] + r1b[j, at(xi * 8, 8), cols]
        u_buf[l + 1, rows_b, cols] = (u_buf[l, rows_b, cols] + val).astype(BF16).astype(F32)
        rdma(6, j, h).start()

    def ev4(j, h):
        wait_pair(5, j, h)
        rdma(7, j, h).start()
        rdma(8, j, h).start()

    def ev5(j, h):
        wait_pair(7, j, h)
        rdma(9, j, h).start()

    def ev6(j, h):
        l, c = split_item(j)
        rdma(9, j, h).wait()

        def finish():
            @pl.loop(0, T // 16)
            def _(i):
                rows = at(c * T + i * 16, 16, 16)
                hid_s[rows, halves[h]] = u_buf[n_layers, rows, halves[h]].astype(BF16)

            out_copy(c, h).start()

        if isinstance(j, int):
            if l == n_layers - 1:
                finish()
        else:
            pl.when(l == n_layers - 1)(finish)

    def guarded(stage, j, *args):
        def run():
            with jax.named_scope(stage.__name__ + "".join(str(a) for a in args)):
                stage(j, *args)

        if isinstance(j, int):
            if 0 <= j < n_items:
                run()
        else:
            pl.when(jnp.logical_and(j >= 0, j < n_items))(run)

    pl.semaphore_wait(barrier, len(relations))

    @pl.loop(0, n_items)
    def _(j):
        guarded(ev6, j - 4, 0)
        guarded(in_norm, j)
        guarded(ev3, j - 2, 1)
        guarded(ev1, j - 1, 1)
        guarded(ev3, j - 2, 0)
        guarded(in_conv, j)
        guarded(ev5, j - 3, 1)
        guarded(ev1, j - 1, 0)
        guarded(in_gate, j)
        guarded(ev4, j - 2, 1)
        guarded(scan_prep, j)
        guarded(ev5, j - 3, 0)
        guarded(scan_a, j)
        guarded(ev2, j - 1, 1)
        guarded(scan_b, j)
        guarded(out_proj, j, 0)
        guarded(ev6, j - 3, 1)
        guarded(ev4, j - 2, 0)
        guarded(out_proj, j, 1)
        guarded(ev2, j - 1, 0)

    z = n_items - 1
    for stage, back, h in (
            (ev6, 3, 0), (ev5, 2, 1), (ev3, 1, 1), (ev6, 2, 1), (ev1, 0, 1), (ev1, 0, 0), (ev5, 2, 0), (ev3, 1, 0),
            (ev6, 2, 0), (ev4, 1, 1), (ev2, 0, 1), (ev2, 0, 0), (ev4, 1, 0), (ev5, 1, 1), (ev3, 0, 1), (ev6, 1, 1),
            (ev3, 0, 0), (ev5, 1, 0), (ev4, 0, 1), (ev6, 1, 0), (ev4, 0, 0), (ev5, 0, 1), (ev6, 0, 1), (ev5, 0, 0),
            (ev6, 0, 0)):
        guarded(stage, z - back, h)

    pltpu.make_async_copy(hid_s, out_ref.at[0], o_sem).wait()


def solution(mesh):
    tp_size = mesh.shape['tp']
    rep_spec = P()
    col_spec = P(None, None, 'tp')
    vec_spec = P(None, 'tp')
    in_specs = (P('dp'), rep_spec, col_spec, col_spec, rep_spec, col_spec, col_spec, rep_spec, vec_spec, rep_spec,
                vec_spec, vec_spec, vec_spec, vec_spec, P(None, 'tp', None))

    def device_forward(hidden, norm_w, w_z, w_x, w_bc, w_dt, conv_x, conv_bc, bias_x, bias_bc, dt_bias, a_log,
                       d_skip, gate_w, w_out):
        n_layers, d_model = norm_w.shape
        n_tok = hidden.shape[1]
        width = w_x.shape[-1]
        n_heads = dt_bias.shape[-1]
        conv_w = width + 2 * STATE
        n_chunks = n_tok // T
        n_items = n_layers * n_chunks
        any_spec = pl.BlockSpec(memory_space=pl.ANY)
        vmem_spec = pl.BlockSpec(memory_space=pltpu.VMEM)
        dma = pltpu.SemaphoreType.DMA
        return pl.pallas_call(
            functools.partial(mixer_kernel, n_layers, n_chunks, width * tp_size),
            out_shape=jax.ShapeDtypeStruct(hidden.shape, BF16),
            in_specs=[any_spec, vmem_spec, any_spec, any_spec, any_spec, any_spec] + [vmem_spec] * 8 + [any_spec],
            out_specs=any_spec,
            scratch_shapes=[
                pltpu.VMEM((n_layers, d_model, conv_w + 128 + width), BF16),
                pltpu.VMEM((n_layers, width, d_model), BF16),
                pltpu.VMEM((n_heads, n_layers, d_model), BF16),
                pltpu.VMEM((16 * n_layers, d_model), F32),
                pltpu.VMEM((n_tok, d_model), BF16),
                pltpu.VMEM((n_layers + 1, n_tok, d_model), F32),
                pltpu.VMEM((T, d_model), F32),
                pltpu.VMEM((n_items, T // 2, d_model), F32),
                pltpu.VMEM((n_items, 16, d_model), F32),
                pltpu.VMEM((n_items, 16, d_model), F32),
                pltpu.VMEM((n_items, 8, d_model), F32),
                pltpu.VMEM((n_items, 8, d_model), F32),
                pltpu.VMEM((T, d_model), BF16),
                pltpu.VMEM((T + 8, conv_w), F32),
                pltpu.VMEM((T, 128 + width), F32),
                pltpu.VMEM((T, width), F32),
                pltpu.VMEM((T, width), F32),
                pltpu.VMEM((T, width), BF16),
                pltpu.VMEM((STATE, width), F32),
                pltpu.VMEM((T, width), F32),
                pltpu.VMEM((T, 128), F32),
                pltpu.VMEM((128, T), F32),
                pltpu.VMEM((T, 128), F32),
                pltpu.VMEM((T, T), F32),
                pltpu.VMEM((STATE, T), F32),
                pltpu.VMEM((T, 128), F32),
                pltpu.VMEM((2, T, T), F32),
                pltpu.VMEM((n_items, 8, T), F32),
                pltpu.VMEM((n_layers, 1, d_model), F32),
                pltpu.VMEM((n_layers, 4, conv_w), F32),
                pltpu.VMEM((n_layers, 1, conv_w), F32),
                pltpu.VMEM((n_layers, 1, 128), F32),
                pltpu.VMEM((n_layers, 1, 128), F32),
                pltpu.VMEM((n_layers, 1, width), F32),
                pltpu.VMEM((n_layers, 1, width), F32),
                dma((n_layers, 3)),
                dma((3,)),
                dma(()),
                dma((n_chunks, 2, 6)),
                dma((n_chunks, 2, 6)),
                dma((n_chunks,)),
                dma((n_chunks,)),
            ],
            compiler_params=pltpu.CompilerParams(
                collective_id=0, has_side_effects=True, vmem_limit_bytes=67043328),
            name="mixer",
        )(hidden, norm_w, w_z, w_x, w_bc, jnp.transpose(w_dt, (2, 0, 1)), conv_x, conv_bc, bias_x, bias_bc, dt_bias,
          a_log, d_skip, gate_w, w_out)

    return jax.shard_map(device_forward, mesh=mesh, in_specs=in_specs, out_specs=P('dp'), check_vma=False)
```

```python
import functools

import jax
import jax.numpy as jnp
from jax import lax
from jax.experimental import pallas as pl
from jax.experimental.pallas import tpu as pltpu
from jax.sharding import PartitionSpec as P

EPS = 1e-5
T = 128
HEAD = 64
STATE = 64
HI = lax.Precision.HIGHEST
F32 = jnp.float32
BF16 = jnp.bfloat16


def mixer_kernel(n_layers, n_chunks, inner_width,
                 hid_ref, norm_hbm, wz_ref, wx_ref, wbc_ref, wdt_ref, convx_hbm, convbc_hbm, biasx_hbm,
                 biasbc_hbm, dtb_hbm, alog_hbm, dskip_hbm, gate_hbm, wout_ref,
                 out_ref,
                 norm_ref, convx_ref, convbc_ref, biasx_ref, biasbc_ref, dtb_ref, alog_ref, dskip_ref, gate_ref,
                 w_in, w_o, wdt_s, wdt_f, hid_s, u_buf, p_buf, r0, r1a, r1b, r2a, r2b, h_buf, c_buf, zd_buf,
                 x_act, v_buf, g_buf, s_buf, cs_buf, acum_s, acumt_s, dt_s, g_s, bt_s, sq_s, f_s, stats,
                 norm_s, cw_s, cb_s, dtb_s, nega_s, dsk_s, gate_s,
                 w_sem, h_sem, par_sem, send_sem, recv_sem, st_send, st_recv):
    d_model = u_buf.shape[2]
    half = d_model // 2
    width = x_act.shape[1]
    n_pairs = width // (2 * HEAD)
    n_heads = dtb_ref.shape[1]
    conv_w = width + 2 * STATE
    n_items = n_layers * n_chunks

    me = lax.axis_index("tp")
    core = lax.rem(me, 2)
    xi = lax.rem(me // 2, 2)
    yi = me // 4

    def peer_id(dx, dy, dc):
        px = xi if dx == 0 else 1 - xi
        py = yi if dy == 0 else 1 - yi
        pc = core if dc == 0 else 1 - core
        return {"tp": py * 4 + px * 2 + pc}

    relations = [(dx, dy, dc) for dx in (0, 1) for dy in (0, 1) for dc in (0, 1)][1:]
    core_peer, x_peer, y_peer = peer_id(0, 0, 1), peer_id(1, 0, 0), peer_id(0, 1, 0)

    def split_item(j):
        if isinstance(j, int):
            return j // n_chunks, j % n_chunks
        return j // n_chunks, lax.rem(j, n_chunks)

    def slot_of(l):
        return l % 2 if isinstance(l, int) else lax.rem(l, 2)

    halves = [slice(0, half), slice(half, d_model)]

    def at(off, size, unit=8):
        return pl.ds(pl.multiple_of(off, unit), size)

    def conv_weight_copies(l):
        return [
            pltpu.make_async_copy(wx_ref.at[l], w_in.at[l, :, pl.ds(0, width)], w_sem.at[l, 0]),
            pltpu.make_async_copy(wbc_ref.at[l], w_in.at[l, :, pl.ds(width, 2 * STATE)], w_sem.at[l, 0]),
        ]

    def gate_weight_copy(l):
        return pltpu.make_async_copy(wz_ref.at[l], w_in.at[l, :, pl.ds(conv_w + 128, width)], w_sem.at[l, 1])

    def out_weight_copy(l):
        return pltpu.make_async_copy(wout_ref.at[l], w_o.at[l], w_sem.at[l, 2])

    def dt_weight_copy():
        return pltpu.make_async_copy(wdt_ref, wdt_s, h_sem.at[2])

    def hid_copy(k):
        rows = pl.ds(0, T) if k == 0 else pl.ds(T, (n_chunks - 1) * T)
        return pltpu.make_async_copy(hid_ref.at[0, rows, :], hid_s.at[rows, :], h_sem.at[k])

    def start_in_weights(l):
        for cp in conv_weight_copies(l):
            cp.start()
        gate_weight_copy(l).start()

    small = [pltpu.make_async_copy(src, dst, par_sem.at[i]) for i, (src, dst) in enumerate((
        (norm_hbm, norm_ref), (convx_hbm, convx_ref), (convbc_hbm, convbc_ref), (biasx_hbm, biasx_ref),
        (biasbc_hbm, biasbc_ref), (dtb_hbm, dtb_ref), (alog_hbm, alog_ref), (dskip_hbm, dskip_ref),
        (gate_hbm, gate_ref)))]

    hid_copy(0).start()
    for cp in small:
        cp.start()
    dt_weight_copy().start()
    start_in_weights(0)

    barrier = pltpu.get_barrier_semaphore()
    for rel in relations:
        pl.semaphore_signal(barrier, inc=1, device_id=peer_id(*rel))

    for cp in small:
        cp.wait()
    lane = lax.broadcasted_iota(jnp.int32, (1, 128), 1)
    for l in range(n_layers):
        norm_s[l] = norm_ref[l:l + 1, :].astype(F32)
        cw_s[l, :, 0:width] = convx_ref[l].astype(F32)
        cw_s[l, :, width:conv_w] = convbc_ref[l].astype(F32)
        cb_s[l, :, 0:width] = biasx_ref[l:l + 1, :].astype(F32)
        cb_s[l, :, width:conv_w] = biasbc_ref[l:l + 1, :].astype(F32)
        gate_s[l] = gate_ref[l:l + 1, :].astype(F32)
        dtb_s[l] = jnp.zeros((1, 128), F32)
        nega_s[l] = jnp.zeros((1, 128), F32)
        dtb_s[l, :, 0:n_heads] = dtb_ref[l:l + 1, :]
        nega_s[l, :, 0:n_heads] = -jnp.exp(alog_ref[l:l + 1, :])
        for p in range(n_pairs):
            d0 = dskip_ref[l:l + 1, 2 * p:2 * p + 1]
            d1 = dskip_ref[l:l + 1, 2 * p + 1:2 * p + 2]
            dsk_s[l, :, 128 * p:128 * (p + 1)] = jnp.where(lane < HEAD, d0, d1)

    def rdma(kind, j, h):
        l, c = split_item(j)
        cols = pl.ds(h * half, half)
        mine = core * (T // 2)
        base = c * T + mine
        group = (kind + 1) // 2
        if kind == 0:
            src, dst, dev = p_buf.at[at((1 - core) * (T // 2), T // 2), cols], r0.at[c, :, cols], core_peer
        elif kind == 1:
            src, dst, dev = r0.at[c, at((1 - xi) * 16, 16), cols], r1a.at[c, :, cols], x_peer
        elif kind == 2:
            src, dst, dev = r0.at[c, at(32 + (1 - yi) * 16, 16), cols], r1b.at[c, :, cols], y_peer
        elif kind == 3:
            src, dst, dev = r1a.at[c, at((1 - yi) * 8, 8), cols], r2a.at[c, :, cols], y_peer
        elif kind == 4:
            src, dst, dev = r1b.at[c, at((1 - xi) * 8, 8), cols], r2b.at[c, :, cols], x_peer
        else:
            off, size, dev = [
                (base + xi * 16 + yi * 8, 8, y_peer),
                (base + 32 + yi * 16 + xi * 8, 8, x_peer),
                (base + xi * 16, 16, x_peer),
                (base + 32 + yi * 16, 16, y_peer),
                (base, T // 2, core_peer),
            ][kind - 5]
            src = u_buf.at[slot_of(l + 1), at(off, size), cols]
            dst = src
        return pltpu.make_async_remote_copy(
            src_ref=src, dst_ref=dst, send_sem=send_sem.at[c, h, group], recv_sem=recv_sem.at[c, h, group],
            device_id=dev, device_id_type=pl.DeviceIdType.MESH)

    def wait_pair(kind, j, h):
        _, c = split_item(j)
        group = (kind + 1) // 2
        size = 32 if kind in (1, 7) else 16
        both = r0.at[c, pl.ds(0, size), pl.ds(h * half, half)]
        pltpu.make_async_copy(both, both, send_sem.at[c, h, group]).wait()
        pltpu.make_async_copy(both, both, recv_sem.at[c, h, group]).wait()

    def stat_copy(r, j):
        _, c = split_item(j)
        return pltpu.make_async_remote_copy(
            src_ref=stats.at[j, pl.ds(0, 1), :], dst_ref=stats.at[j, pl.ds(r + 1, 1), :],
            send_sem=st_send.at[c], recv_sem=st_recv.at[c],
            device_id=peer_id(*relations[r]), device_id_type=pl.DeviceIdType.MESH)

    def wait_stats(j):
        _, c = split_item(j)
        rows = stats.at[j, pl.ds(1, len(relations)), :]
        pltpu.make_async_copy(rows, rows, st_send.at[c]).wait()
        pltpu.make_async_copy(rows, rows, st_recv.at[c]).wait()

    def in_norm(j):
        l, c = split_item(j)
        base = c * T

        @pl.when(j == 0)
        def _():
            hid_copy(0).wait()

        @pl.when(j == 1)
        def _():
            hid_copy(1).wait()
            for k in range(1, n_layers):
                start_in_weights(k)
                out_weight_copy(k).start()

        def squares(load):
            @pl.loop(0, T // 16)
            def _(i):
                acc = jnp.zeros((16, 128), F32)
                for n in range(0, d_model, 128):
                    u = load(base + i * 16, slice(n, n + 128))
                    acc = acc + u * u
                sq_s[at(i * 16, 16, 16), :] = acc

        def load_hidden(off, cols):
            u = hid_s[at(off, 16, 16), cols].astype(F32)
            u_buf[0, at(off, 16, 16), cols] = u
            return u

        def load_u(off, cols):
            return u_buf[slot_of(l), at(off, 16, 16), cols]

        pl.when(l == 0)(lambda: squares(load_hidden))
        pl.when(l > 0)(lambda: squares(load_u))
        ms = jnp.sum(sq_s[...], axis=-1, keepdims=True) * (1.0 / d_model)
        sq_s[...] = jnp.broadcast_to(lax.rsqrt(ms + EPS), (T, 128))

        @pl.loop(0, T // 16)
        def _(i):
            rs = sq_s[at(i * 16, 16, 16), :]
            for n in range(0, d_model, 128):
                cols = slice(n, n + 128)
                h = load_u(base + i * 16, cols) * rs * norm_s[l, :, cols]
                h_buf[at(i * 16, 16, 16), cols] = h.astype(BF16)

        @pl.when(c == 0)
        def _():
            c_buf[0:8, :] = jnp.zeros((8, conv_w), F32)
            s_buf[...] = jnp.zeros_like(s_buf)

        @pl.when(c > 0)
        def _():
            c_buf[0:8, :] = c_buf[T:T + 8, :]

    def in_conv(j):
        l, c = split_item(j)

        @pl.when(j == 0)
        def _():
            dt_weight_copy().wait()
            for k in range(n_layers):
                wdt_f[16 * k + 8:16 * k + 16, :] = jnp.zeros((8, d_model), F32)
            for n in range(n_heads):
                rows = wdt_s[n].astype(F32)
                for k in range(n_layers):
                    wdt_f[16 * k + n:16 * k + n + 1, :] = rows[k:k + 1, :]

        @pl.when(c == 0)
        def _():
            w_in[l, :, conv_w:conv_w + 128] = jnp.zeros((d_model, 128), BF16)
            w_in[l, :, conv_w:conv_w + 16] = wdt_f[at(16 * l, 16), :].T.astype(BF16)
            both = w_in.at[l, :, pl.ds(0, conv_w)]
            pltpu.make_async_copy(both, both, w_sem.at[l, 0]).wait()

        h = h_buf[...]
        for n in range(0, conv_w, 256):
            r = jnp.dot(h, w_in[l, :, n:n + 256], preferred_element_type=F32)
            c_buf[8:8 + T, n:n + 256] = r.astype(BF16).astype(F32)

    def in_gate(j):
        l, c = split_item(j)

        @pl.when(c == 0)
        def _():
            gate_weight_copy(l).wait()

        @pl.when(j == 0)
        def _():
            out_weight_copy(0).start()
            hid_copy(1).start()

        h = h_buf[...]
        for n in range(0, width + 128, 256):
            r = jnp.dot(h, w_in[l, :, conv_w + n:conv_w + n + 256], preferred_element_type=F32)
            zd_buf[:, n:n + 256] = r.astype(BF16).astype(F32)

    def scan_prep(j):
        l, _ = split_item(j)
        b_act = None
        for n in range(0, conv_w, 128):
            cols = slice(n, n + 128)
            acc = cb_s[l, :, cols] + c_buf[5:5 + T, cols] * cw_s[l, 0:1, cols]
            for k in range(1, 4):
                acc = acc + c_buf[5 + k:5 + k + T, cols] * cw_s[l, k:k + 1, cols]
            act = acc * jax.nn.sigmoid(acc)
            if n < width:
                x_act[:, cols] = act
            else:
                b_act = act
        bt = b_act.T[0:STATE, :]
        c_mat = b_act[:, STATE:2 * STATE]
        bt_s[...] = bt
        g_s[...] = jnp.dot(c_mat, bt, precision=HI, preferred_element_type=F32)
        cs_buf[...] = jnp.dot(c_mat, s_buf[...], precision=HI, preferred_element_type=F32)
        dt = jax.nn.softplus(zd_buf[:, 0:128] + dtb_s[l])
        a = dt * nega_s[l]
        row = lax.broadcasted_iota(jnp.int32, (T, T), 0)
        col = lax.broadcasted_iota(jnp.int32, (T, T), 1)
        tril = jnp.where(row >= col, 1.0, 0.0).astype(F32)
        acum = jnp.dot(tril, a, precision=HI, preferred_element_type=F32)
        dt_s[...] = dt
        acum_s[...] = acum
        acumt_s[...] = acum.T

    def scan_pairs(j, pairs):
        l, _ = split_item(j)
        row = lax.broadcasted_iota(jnp.int32, (T, T), 0)
        col = lax.broadcasted_iota(jnp.int32, (T, T), 1)
        causal = row >= col
        low = col < HEAD
        low_row = lane < HEAD
        g = g_s[...]
        bt = bt_s[...]
        sq = jnp.zeros((T, 128), F32)
        for p in pairs:
            h0, h1 = 2 * p, 2 * p + 1
            cols = slice(128 * p, 128 * (p + 1))
            a0 = jnp.broadcast_to(acum_s[:, h0:h0 + 1], (T, T))
            a1 = jnp.broadcast_to(acum_s[:, h1:h1 + 1], (T, T))
            m0 = jnp.where(causal, jnp.exp(jnp.minimum(a0 - acumt_s[h0:h0 + 1, :], 0.0)), 0.0) * g
            m1 = jnp.where(causal, jnp.exp(jnp.minimum(a1 - acumt_s[h1:h1 + 1, :], 0.0)), 0.0) * g
            dt = jnp.where(low, dt_s[:, h0:h0 + 1], dt_s[:, h1:h1 + 1])
            x = x_act[:, cols]
            xd = x * dt
            both = jnp.concatenate([m0, m1], axis=1)
            split = jnp.concatenate([jnp.where(low, xd, 0.0), jnp.where(low, 0.0, xd)], axis=0)
            y = jnp.dot(both, split, precision=HI, preferred_element_type=F32)
            ap = jnp.where(low, a0, a1)
            last = jnp.where(low_row, acum_s[T - 1:T, h0:h0 + 1], acum_s[T - 1:T, h1:h1 + 1])
            y = y + cs_buf[:, cols] * jnp.exp(ap)
            xt = xd * jnp.exp(last - ap)
            s_buf[:, cols] = s_buf[:, cols] * jnp.exp(last) + jnp.dot(bt, xt, precision=HI, preferred_element_type=F32)
            y = y + dsk_s[l, :, cols] * x
            z = zd_buf[:, 128 + 128 * p:256 + 128 * p]
            v = y * (z * jax.nn.sigmoid(z))
            v_buf[:, cols] = v
            sq = sq + v * v
        return sq

    first_pairs = (n_pairs + 1) // 2

    def scan_a(j):
        sq_s[...] = scan_pairs(j, range(first_pairs))

    def scan_b(j):
        l, _ = split_item(j)
        sq = sq_s[...] + scan_pairs(j, range(first_pairs, n_pairs))
        ones = jnp.ones((8, 128), F32)
        part = lax.dot_general(ones, sq, (((1,), (1,)), ((), ())), precision=HI, preferred_element_type=F32)
        stats[j, 0:1, :] = part[0:1, :]
        for r in range(len(relations)):
            stat_copy(r, j).start()
        own = lax.rsqrt(jnp.sum(sq, axis=1, keepdims=True) * (1.0 / width) + EPS)
        for p in range(n_pairs):
            cols = slice(128 * p, 128 * (p + 1))
            g_buf[:, cols] = (v_buf[:, cols] * own * gate_s[l, :, cols]).astype(BF16)

    def out_proj(j, h):
        l, c = split_item(j)
        if h == 0:
            @pl.when(c == 0)
            def _():
                out_weight_copy(l).wait()

        g = g_buf[...]
        for n in range(h * half, (h + 1) * half, 256):
            p_buf[:, n:n + 256] = jnp.dot(g, w_o[l, :, n:n + 256], preferred_element_type=F32)
        rdma(0, j, h).start()

    def factors(j):
        wait_stats(j)
        st = stats[j]
        rs = lax.rsqrt(jnp.sum(st, axis=0, keepdims=True) * (1.0 / inner_width) + EPS)
        for k in range(2):
            own = lax.rsqrt(st[k:k + 1, :] * (1.0 / width) + EPS)
            f = rs / jnp.maximum(own, 1e-30)
            f_s[k] = jnp.broadcast_to(f, (T, T)).T

    def ev1(j, h):
        _, c = split_item(j)
        if h == 1:
            factors(j)
        mine = core * (T // 2)
        rdma(0, j, h).wait()

        def add(off):
            f_me = f_s[0, at(mine + off, 16), :]
            f_peer = f_s[1, at(mine + off, 16), :]
            for n in range(h * half, (h + 1) * half, 128):
                cols = slice(n, n + 128)
                r0[c, at(off, 16), cols] = r0[c, at(off, 16), cols] * f_peer + p_buf[at(mine + off, 16), cols] * f_me

        add((1 - xi) * 16)
        rdma(1, j, h).start()
        add(32 + (1 - yi) * 16)
        rdma(2, j, h).start()
        add(xi * 16)
        add(32 + yi * 16)

    def ev2(j, h):
        _, c = split_item(j)
        cols = halves[h]
        wait_pair(1, j, h)
        r1a[c, :, cols] += r0[c, at(xi * 16, 16), cols]
        rdma(3, j, h).start()
        r1b[c, :, cols] += r0[c, at(32 + yi * 16, 16), cols]
        rdma(4, j, h).start()

    def ev3(j, h):
        l, c = split_item(j)
        cols = halves[h]
        base = c * T + core * (T // 2)
        rows_a = at(base + xi * 16 + yi * 8, 8)
        rows_b = at(base + 32 + yi * 16 + xi * 8, 8)
        wait_pair(3, j, h)
        val = r2a[c, :, cols] + r1a[c, at(yi * 8, 8), cols]
        u_buf[slot_of(l + 1), rows_a, cols] = (u_buf[slot_of(l), rows_a, cols] + val).astype(BF16).astype(F32)
        rdma(5, j, h).start()
        val = r2b[c, :, cols] + r1b[c, at(xi * 8, 8), cols]
        u_buf[slot_of(l + 1), rows_b, cols] = (u_buf[slot_of(l), rows_b, cols] + val).astype(BF16).astype(F32)
        rdma(6, j, h).start()

    def ev4(j, h):
        wait_pair(5, j, h)
        rdma(7, j, h).start()
        rdma(8, j, h).start()

    def ev5(j, h):
        wait_pair(7, j, h)
        rdma(9, j, h).start()

    def ev6(j, h):
        l, c = split_item(j)
        rdma(9, j, h).wait()

        def finish():
            @pl.loop(0, T // 16)
            def _(i):
                rows = at(c * T + i * 16, 16, 16)
                out_ref[0, rows, halves[h]] = u_buf[n_layers % 2, rows, halves[h]].astype(BF16)

        if isinstance(j, int):
            if l == n_layers - 1:
                finish()
        else:
            pl.when(l == n_layers - 1)(finish)

    def guarded(stage, j, *args):
        def run():
            with jax.named_scope(stage.__name__ + "".join(str(a) for a in args)):
                stage(j, *args)

        if isinstance(j, int):
            if 0 <= j < n_items:
                run()
        else:
            pl.when(jnp.logical_and(j >= 0, j < n_items))(run)

    pl.semaphore_wait(barrier, len(relations))

    @pl.loop(0, n_items)
    def _(j):
        guarded(ev6, j - 4, 0)
        guarded(in_norm, j)
        guarded(ev3, j - 2, 1)
        guarded(ev1, j - 1, 1)
        guarded(ev3, j - 2, 0)
        guarded(in_conv, j)
        guarded(ev5, j - 3, 1)
        guarded(ev1, j - 1, 0)
        guarded(in_gate, j)
        guarded(ev4, j - 2, 1)
        guarded(scan_prep, j)
        guarded(ev5, j - 3, 0)
        guarded(scan_a, j)
        guarded(ev2, j - 1, 1)
        guarded(scan_b, j)
        guarded(out_proj, j, 0)
        guarded(ev6, j - 3, 1)
        guarded(ev4, j - 2, 0)
        guarded(out_proj, j, 1)
        guarded(ev2, j - 1, 0)

    z = n_items - 1
    for stage, back, h in (
            (ev6, 3, 0), (ev5, 2, 1), (ev3, 1, 1), (ev6, 2, 1), (ev1, 0, 1), (ev1, 0, 0), (ev5, 2, 0), (ev3, 1, 0),
            (ev6, 2, 0), (ev4, 1, 1), (ev2, 0, 1), (ev2, 0, 0), (ev4, 1, 0), (ev5, 1, 1), (ev3, 0, 1), (ev6, 1, 1),
            (ev3, 0, 0), (ev5, 1, 0), (ev4, 0, 1), (ev6, 1, 0), (ev4, 0, 0), (ev5, 0, 1), (ev6, 0, 1), (ev5, 0, 0),
            (ev6, 0, 0)):
        guarded(stage, z - back, h)


def solution(mesh):
    tp_size = mesh.shape['tp']
    rep_spec = P()
    col_spec = P(None, None, 'tp')
    vec_spec = P(None, 'tp')
    in_specs = (P('dp'), rep_spec, col_spec, col_spec, rep_spec, col_spec, col_spec, rep_spec, vec_spec, rep_spec,
                vec_spec, vec_spec, vec_spec, vec_spec, P(None, 'tp', None))

    def device_forward(hidden, norm_w, w_z, w_x, w_bc, w_dt, conv_x, conv_bc, bias_x, bias_bc, dt_bias, a_log,
                       d_skip, gate_w, w_out):
        n_layers, d_model = norm_w.shape
        n_tok = hidden.shape[1]
        width = w_x.shape[-1]
        n_heads = dt_bias.shape[-1]
        conv_w = width + 2 * STATE
        n_chunks = n_tok // T
        n_items = n_layers * n_chunks
        any_spec = pl.BlockSpec(memory_space=pltpu.HBM)
        vmem_spec = pl.BlockSpec(memory_space=pltpu.VMEM)
        dma = pltpu.SemaphoreType.DMA
        return pl.pallas_call(
            functools.partial(mixer_kernel, n_layers, n_chunks, width * tp_size),
            out_shape=jax.ShapeDtypeStruct(hidden.shape, BF16),
            in_specs=[any_spec] * 15,
            out_specs=vmem_spec,
            scratch_shapes=[
                pltpu.VMEM(norm_w.shape, BF16),
                pltpu.VMEM(conv_x.shape, BF16),
                pltpu.VMEM(conv_bc.shape, BF16),
                pltpu.VMEM(bias_x.shape, BF16),
                pltpu.VMEM(bias_bc.shape, BF16),
                pltpu.VMEM(dt_bias.shape, F32),
                pltpu.VMEM(a_log.shape, F32),
                pltpu.VMEM(d_skip.shape, F32),
                pltpu.VMEM(gate_w.shape, BF16),
                pltpu.VMEM((n_layers, d_model, conv_w + 128 + width), BF16),
                pltpu.VMEM((n_layers, width, d_model), BF16),
                pltpu.VMEM((n_heads, n_layers, d_model), BF16),
                pltpu.VMEM((16 * n_layers, d_model), F32),
                pltpu.VMEM((n_tok, d_model), BF16),
                pltpu.VMEM((2, n_tok, d_model), F32),
                pltpu.VMEM((T, d_model), F32),
                pltpu.VMEM((n_chunks, T // 2, d_model), F32),
                pltpu.VMEM((n_chunks, 16, d_model), F32),
                pltpu.VMEM((n_chunks, 16, d_model), F32),
                pltpu.VMEM((n_chunks, 8, d_model), F32),
                pltpu.VMEM((n_chunks, 8, d_model), F32),
                pltpu.VMEM((T, d_model), BF16),
                pltpu.VMEM((T + 8, conv_w), F32),
                pltpu.VMEM((T, 128 + width), F32),
                pltpu.VMEM((T, width), F32),
                pltpu.VMEM((T, width), F32),
                pltpu.VMEM((T, width), BF16),
                pltpu.VMEM((STATE, width), F32),
                pltpu.VMEM((T, width), F32),
                pltpu.VMEM((T, 128), F32),
                pltpu.VMEM((128, T), F32),
                pltpu.VMEM((T, 128), F32),
                pltpu.VMEM((T, T), F32),
                pltpu.VMEM((STATE, T), F32),
                pltpu.VMEM((T, 128), F32),
                pltpu.VMEM((2, T, T), F32),
                pltpu.VMEM((n_items, 8, T), F32),
                pltpu.VMEM((n_layers, 1, d_model), F32),
                pltpu.VMEM((n_layers, 4, conv_w), F32),
                pltpu.VMEM((n_layers, 1, conv_w), F32),
                pltpu.VMEM((n_layers, 1, 128), F32),
                pltpu.VMEM((n_layers, 1, 128), F32),
                pltpu.VMEM((n_layers, 1, width), F32),
                pltpu.VMEM((n_layers, 1, width), F32),
                dma((n_layers, 3)),
                dma((3,)),
                dma((9,)),
                dma((n_chunks, 2, 6)),
                dma((n_chunks, 2, 6)),
                dma((n_chunks,)),
                dma((n_chunks,)),
            ],
            compiler_params=pltpu.CompilerParams(
                collective_id=0, has_side_effects=True, vmem_limit_bytes=50000000),
            name="mixer",
        )(*[pltpu.with_memory_space_constraint(arg, pltpu.HBM) for arg in (
            hidden, norm_w, w_z, w_x, w_bc, jnp.transpose(w_dt, (2, 0, 1)), conv_x, conv_bc, bias_x, bias_bc, dt_bias,
            a_log, d_skip, gate_w, w_out)])

    return jax.shard_map(device_forward, mesh=mesh, in_specs=in_specs, out_specs=P('dp'), check_vma=False)
```

```python
import functools

import jax
import jax.numpy as jnp
from jax import lax
from jax.experimental import pallas as pl
from jax.experimental.pallas import tpu as pltpu
from jax.sharding import PartitionSpec as P

EPS = 1e-5
T = 128
HEAD = 64
STATE = 64
HI = lax.Precision.HIGHEST
F32 = jnp.float32
BF16 = jnp.bfloat16

SLOTS = (
    ((4, 0, 3, 0, (), ()), (3, 1, 2, 0, (1,), ()),),
    ((2, 1, 2, 0, (2,), ()), (5, 0, 3, 0, (1,), ()), (1, 0, 1, 1, (), (0, 2)), (1, 1, 1, 0, (1,), ()), (1, 1, 1, 0, (), (0, 1, 2)),),
    ((3, 1, 2, 0, (), (0, 1, 2)), (1, 0, 1, 1, (2,), ()), (3, 0, 2, 0, (0,), ()), (1, 1, 1, 1, (0,), ()),),
    ((5, 1, 3, 0, (2,), ()),),
    ((1, 0, 1, 0, (0,), ()), (5, 1, 3, 0, (), (0, 2)), (2, 0, 1, 0, (1,), ()), (6, 1, 3, 0, (), (0, 1)), (5, 0, 3, 0, (2,), ()), (3, 1, 2, 0, (2,), ()), (3, 0, 2, 0, (), (0,)), (5, 1, 3, 0, (0,), ()),),
    ((6, 0, 3, 0, (1,), ()), (1, 1, 1, 0, (2,), ()), (5, 0, 3, 0, (0,), ()), (2, 0, 1, 0, (), (0, 1)),),
    ((2, 1, 1, 0, (), (1, 2)), (5, 0, 3, 0, (), (0, 1, 2)), (6, 1, 3, 0, (1,), ()), (4, 1, 2, 0, (), (0, 2)),),
    ((6, 0, 3, 0, (0,), ()), (6, 0, 3, 0, (), (0, 1, 2)), (2, 1, 1, 0, (1,), ()),),
    ((2, 0, 1, 0, (0,), ()), (4, 1, 2, 0, (0,), ()), (4, 1, 2, 0, (2,), ()), (6, 1, 3, 0, (0,), ()), (6, 0, 3, 0, (2,), ()), (3, 1, 1, 0, (0,), ()),),
)
DRAIN = ((4, 0, 5, 0), (1, 1, 7, 1), (5, 1, 5, 0), (1, 0, 7, 0), (2, 1, 7, 0), (3, 0, 6, 0), (3, 1, 6, 0), (5, 0, 5, 0), (2, 0, 7, 0), (3, 1, 7, 0), (4, 0, 6, 0), (3, 0, 7, 0), (6, 1, 5, 0), (4, 1, 6, 0), (5, 0, 6, 0), (4, 1, 7, 0), (4, 0, 7, 0), (6, 0, 6, 0), (5, 1, 6, 0), (5, 1, 7, 0), (5, 0, 7, 0), (6, 1, 6, 0), (6, 0, 5, 0), (6, 1, 7, 0), (6, 0, 7, 0))


def mixer_kernel(n_layers, n_chunks, inner_width,
                 hid_ref, norm_hbm, wz_ref, wx_ref, wbc_ref, wdt_ref, convx_hbm, convbc_hbm, biasx_hbm,
                 biasbc_hbm, dtb_hbm, alog_hbm, dskip_hbm, gate_hbm, wout_ref,
                 out_ref,
                 norm_ref, convx_ref, convbc_ref, biasx_ref, biasbc_ref, dtb_ref, alog_ref, dskip_ref, gate_ref,
                 w_in, w_o, wdt_s, wdt_f, hid_s, u_buf, p_buf, r0, r1a, r1b, r2a, r2b, h_buf, c_buf, zd_buf,
                 x_act, v_buf, g_buf, s_buf, cs_buf, acum_s, acumt_s, dt_s, g_s, bt_s, sq_s, f_s, stats,
                 norm_s, cw_s, cb_s, dtb_s, nega_s, dsk_s, gate_s,
                 w_sem, h_sem, par_sem, send_sem, recv_sem, st_send, st_recv):
    d_model = u_buf.shape[2]
    half = d_model // 2
    width = x_act.shape[1]
    n_pairs = width // (2 * HEAD)
    n_heads = dtb_ref.shape[1]
    conv_w = width + 2 * STATE
    n_items = n_layers * n_chunks

    me = lax.axis_index("tp")
    core = lax.rem(me, 2)
    xi = lax.rem(me // 2, 2)
    yi = me // 4

    def peer_id(dx, dy, dc):
        px = xi if dx == 0 else 1 - xi
        py = yi if dy == 0 else 1 - yi
        pc = core if dc == 0 else 1 - core
        return {"tp": py * 4 + px * 2 + pc}

    relations = [(dx, dy, dc) for dx in (0, 1) for dy in (0, 1) for dc in (0, 1)][1:]
    core_peer, x_peer, y_peer = peer_id(0, 0, 1), peer_id(1, 0, 0), peer_id(0, 1, 0)

    def split_item(j):
        if isinstance(j, int):
            return j // n_chunks, j % n_chunks
        return j // n_chunks, lax.rem(j, n_chunks)

    def slot_of(l):
        return l % 2 if isinstance(l, int) else lax.rem(l, 2)

    halves = [slice(0, half), slice(half, d_model)]

    def at(off, size, unit=8):
        return pl.ds(pl.multiple_of(off, unit), size)

    def conv_weight_copies(l):
        return [
            pltpu.make_async_copy(wx_ref.at[l], w_in.at[l, :, pl.ds(0, width)], w_sem.at[l, 0]),
            pltpu.make_async_copy(wbc_ref.at[l], w_in.at[l, :, pl.ds(width, 2 * STATE)], w_sem.at[l, 0]),
        ]

    def gate_weight_copy(l):
        return pltpu.make_async_copy(wz_ref.at[l], w_in.at[l, :, pl.ds(conv_w + 128, width)], w_sem.at[l, 1])

    def out_weight_copy(l):
        return pltpu.make_async_copy(wout_ref.at[l], w_o.at[l], w_sem.at[l, 2])

    def dt_weight_copy():
        return pltpu.make_async_copy(wdt_ref, wdt_s, h_sem.at[2])

    def hid_copy(k):
        rows = pl.ds(0, T) if k == 0 else pl.ds(T, (n_chunks - 1) * T)
        return pltpu.make_async_copy(hid_ref.at[0, rows, :], hid_s.at[rows, :], h_sem.at[k])

    def start_in_weights(l):
        for cp in conv_weight_copies(l):
            cp.start()
        gate_weight_copy(l).start()

    small = [pltpu.make_async_copy(src, dst, par_sem.at[i]) for i, (src, dst) in enumerate((
        (norm_hbm, norm_ref), (convx_hbm, convx_ref), (convbc_hbm, convbc_ref), (biasx_hbm, biasx_ref),
        (biasbc_hbm, biasbc_ref), (dtb_hbm, dtb_ref), (alog_hbm, alog_ref), (dskip_hbm, dskip_ref),
        (gate_hbm, gate_ref)))]

    hid_copy(0).start()
    small[0].start()
    dt_weight_copy().start()
    for cp in conv_weight_copies(0):
        cp.start()
    for cp in small[1:]:
        cp.start()

    barrier = pltpu.get_barrier_semaphore()
    for rel in relations:
        pl.semaphore_signal(barrier, inc=1, device_id=peer_id(*rel))

    lane = lax.broadcasted_iota(jnp.int32, (1, 128), 1)
    small[0].wait()
    gate_weight_copy(0).start()
    for l in range(n_layers):
        norm_s[l] = norm_ref[l:l + 1, :].astype(F32)

    def small_parameters():
        for cp in small[1:]:
            cp.wait()
        for l in range(n_layers):
            cw_s[l, :, 0:width] = convx_ref[l].astype(F32)
            cw_s[l, :, width:conv_w] = convbc_ref[l].astype(F32)
            cb_s[l, :, 0:width] = biasx_ref[l:l + 1, :].astype(F32)
            cb_s[l, :, width:conv_w] = biasbc_ref[l:l + 1, :].astype(F32)
            gate_s[l] = gate_ref[l:l + 1, :].astype(F32)
            dtb_s[l] = jnp.zeros((1, 128), F32)
            nega_s[l] = jnp.zeros((1, 128), F32)
            dtb_s[l, :, 0:n_heads] = dtb_ref[l:l + 1, :]
            nega_s[l, :, 0:n_heads] = -jnp.exp(alog_ref[l:l + 1, :])
            for p in range(n_pairs):
                d0 = dskip_ref[l:l + 1, 2 * p:2 * p + 1]
                d1 = dskip_ref[l:l + 1, 2 * p + 1:2 * p + 2]
                dsk_s[l, :, 128 * p:128 * (p + 1)] = jnp.where(lane < HEAD, d0, d1)

    def rdma(kind, j, h):
        l, c = split_item(j)
        cols = pl.ds(h * half, half)
        mine = core * (T // 2)
        base = c * T + mine
        group = (kind + 1) // 2
        if kind == 0:
            src, dst, dev = p_buf.at[at((1 - core) * (T // 2), T // 2), cols], r0.at[c, :, cols], core_peer
        elif kind == 1:
            src, dst, dev = r0.at[c, at((1 - xi) * 16, 16), cols], r1a.at[c, :, cols], x_peer
        elif kind == 2:
            src, dst, dev = r0.at[c, at(32 + (1 - yi) * 16, 16), cols], r1b.at[c, :, cols], y_peer
        elif kind == 3:
            src, dst, dev = r1a.at[c, at((1 - yi) * 8, 8), cols], r2a.at[c, :, cols], y_peer
        elif kind == 4:
            src, dst, dev = r1b.at[c, at((1 - xi) * 8, 8), cols], r2b.at[c, :, cols], x_peer
        else:
            off, size, dev = [
                (base + xi * 16 + yi * 8, 8, y_peer),
                (base + 32 + yi * 16 + xi * 8, 8, x_peer),
                (base + xi * 16, 16, x_peer),
                (base + 32 + yi * 16, 16, y_peer),
                (base, T // 2, core_peer),
            ][kind - 5]
            src = u_buf.at[slot_of(l + 1), at(off, size), cols]
            dst = src
        return pltpu.make_async_remote_copy(
            src_ref=src, dst_ref=dst, send_sem=send_sem.at[c, h, group], recv_sem=recv_sem.at[c, h, group],
            device_id=dev, device_id_type=pl.DeviceIdType.MESH)

    def wait_pair(kind, j, h):
        _, c = split_item(j)
        group = (kind + 1) // 2
        size = 32 if kind in (1, 7) else 16
        both = r0.at[c, pl.ds(0, size), pl.ds(h * half, half)]
        pltpu.make_async_copy(both, both, send_sem.at[c, h, group]).wait()
        pltpu.make_async_copy(both, both, recv_sem.at[c, h, group]).wait()

    def stat_copy(r, j):
        _, c = split_item(j)
        return pltpu.make_async_remote_copy(
            src_ref=stats.at[j, pl.ds(0, 1), :], dst_ref=stats.at[j, pl.ds(r + 1, 1), :],
            send_sem=st_send.at[c], recv_sem=st_recv.at[c],
            device_id=peer_id(*relations[r]), device_id_type=pl.DeviceIdType.MESH)

    def wait_stats(j):
        _, c = split_item(j)
        rows = stats.at[j, pl.ds(1, len(relations)), :]
        pltpu.make_async_copy(rows, rows, st_send.at[c]).wait()
        pltpu.make_async_copy(rows, rows, st_recv.at[c]).wait()

    def in_norm(j):
        l, c = split_item(j)
        base = c * T

        @pl.when(j == 0)
        def _():
            hid_copy(0).wait()

        @pl.when(j == 1)
        def _():
            hid_copy(1).wait()
            for k in range(1, n_layers):
                start_in_weights(k)
                out_weight_copy(k).start()

        def squares(load):
            @pl.loop(0, T // 16)
            def _(i):
                acc = jnp.zeros((16, 128), F32)
                for n in range(0, d_model, 128):
                    u = load(base + i * 16, slice(n, n + 128))
                    acc = acc + u * u
                sq_s[at(i * 16, 16, 16), :] = acc

        def load_hidden(off, cols):
            u = hid_s[at(off, 16, 16), cols].astype(F32)
            u_buf[0, at(off, 16, 16), cols] = u
            return u

        def load_u(off, cols):
            return u_buf[slot_of(l), at(off, 16, 16), cols]

        pl.when(l == 0)(lambda: squares(load_hidden))
        pl.when(l > 0)(lambda: squares(load_u))
        ms = jnp.sum(sq_s[...], axis=-1, keepdims=True) * (1.0 / d_model)
        sq_s[...] = jnp.broadcast_to(lax.rsqrt(ms + EPS), (T, 128))

        @pl.loop(0, T // 16)
        def _(i):
            rs = sq_s[at(i * 16, 16, 16), :]
            for n in range(0, d_model, 128):
                cols = slice(n, n + 128)
                h = load_u(base + i * 16, cols) * rs * norm_s[l, :, cols]
                h_buf[at(i * 16, 16, 16), cols] = h.astype(BF16)

        @pl.when(c == 0)
        def _():
            c_buf[0:8, :] = jnp.zeros((8, conv_w), F32)
            s_buf[...] = jnp.zeros_like(s_buf)

        @pl.when(c > 0)
        def _():
            c_buf[0:8, :] = c_buf[T:T + 8, :]

    def in_conv(j):
        l, c = split_item(j)

        @pl.when(c == 0)
        def _():
            both = w_in.at[l, :, pl.ds(0, conv_w)]
            pltpu.make_async_copy(both, both, w_sem.at[l, 0]).wait()

        h = h_buf[...]
        for n in range(0, conv_w, 256):
            r = jnp.dot(h, w_in[l, :, n:n + 256], preferred_element_type=F32)
            c_buf[8:8 + T, n:n + 256] = r.astype(BF16).astype(F32)

    def in_gate(j):
        l, c = split_item(j)

        @pl.when(j == 0)
        def _():
            dt_weight_copy().wait()
            for k in range(n_layers):
                wdt_f[16 * k + 8:16 * k + 16, :] = jnp.zeros((8, d_model), F32)
            for n in range(n_heads):
                rows = wdt_s[n].astype(F32)
                for k in range(n_layers):
                    wdt_f[16 * k + n:16 * k + n + 1, :] = rows[k:k + 1, :]

        @pl.when(c == 0)
        def _():
            w_in[l, :, conv_w:conv_w + 128] = jnp.zeros((d_model, 128), BF16)
            w_in[l, :, conv_w:conv_w + 16] = wdt_f[at(16 * l, 16), :].T.astype(BF16)
            gate_weight_copy(l).wait()

        @pl.when(j == 0)
        def _():
            out_weight_copy(0).start()
            hid_copy(1).start()
            small_parameters()

        h = h_buf[...]
        for n in range(0, width + 128, 256):
            r = jnp.dot(h, w_in[l, :, conv_w + n:conv_w + n + 256], preferred_element_type=F32)
            zd_buf[:, n:n + 256] = r.astype(BF16).astype(F32)

    def scan_prep(j):
        l, _ = split_item(j)
        b_act = None
        for n in range(0, conv_w, 128):
            cols = slice(n, n + 128)
            acc = cb_s[l, :, cols] + c_buf[5:5 + T, cols] * cw_s[l, 0:1, cols]
            for k in range(1, 4):
                acc = acc + c_buf[5 + k:5 + k + T, cols] * cw_s[l, k:k + 1, cols]
            act = acc * jax.nn.sigmoid(acc)
            if n < width:
                x_act[:, cols] = act
            else:
                b_act = act
        bt = b_act.T[0:STATE, :]
        c_mat = b_act[:, STATE:2 * STATE]
        bt_s[...] = bt
        g_s[...] = jnp.dot(c_mat, bt, precision=HI, preferred_element_type=F32)
        cs_buf[...] = jnp.dot(c_mat, s_buf[...], precision=HI, preferred_element_type=F32)
        dt = jax.nn.softplus(zd_buf[:, 0:128] + dtb_s[l])
        a = dt * nega_s[l]
        row = lax.broadcasted_iota(jnp.int32, (T, T), 0)
        col = lax.broadcasted_iota(jnp.int32, (T, T), 1)
        tril = jnp.where(row >= col, 1.0, 0.0).astype(F32)
        acum = jnp.dot(tril, a, precision=HI, preferred_element_type=F32)
        dt_s[...] = dt
        acum_s[...] = acum
        acumt_s[...] = acum.T

    def scan_pairs(j, pairs):
        l, _ = split_item(j)
        row = lax.broadcasted_iota(jnp.int32, (T, T), 0)
        col = lax.broadcasted_iota(jnp.int32, (T, T), 1)
        causal = row >= col
        low = col < HEAD
        low_row = lane < HEAD
        g = g_s[...]
        bt = bt_s[...]
        sq = jnp.zeros((T, 128), F32)
        for p in pairs:
            h0, h1 = 2 * p, 2 * p + 1
            cols = slice(128 * p, 128 * (p + 1))
            a0 = jnp.broadcast_to(acum_s[:, h0:h0 + 1], (T, T))
            a1 = jnp.broadcast_to(acum_s[:, h1:h1 + 1], (T, T))
            m0 = jnp.where(causal, jnp.exp(jnp.minimum(a0 - acumt_s[h0:h0 + 1, :], 0.0)), 0.0) * g
            m1 = jnp.where(causal, jnp.exp(jnp.minimum(a1 - acumt_s[h1:h1 + 1, :], 0.0)), 0.0) * g
            dt = jnp.where(low, dt_s[:, h0:h0 + 1], dt_s[:, h1:h1 + 1])
            x = x_act[:, cols]
            xd = x * dt
            both = jnp.concatenate([m0, m1], axis=1)
            split = jnp.concatenate([jnp.where(low, xd, 0.0), jnp.where(low, 0.0, xd)], axis=0)
            y = jnp.dot(both, split, precision=HI, preferred_element_type=F32)
            ap = jnp.where(low, a0, a1)
            last = jnp.where(low_row, acum_s[T - 1:T, h0:h0 + 1], acum_s[T - 1:T, h1:h1 + 1])
            y = y + cs_buf[:, cols] * jnp.exp(ap)
            xt = xd * jnp.exp(last - ap)
            s_buf[:, cols] = s_buf[:, cols] * jnp.exp(last) + jnp.dot(bt, xt, precision=HI, preferred_element_type=F32)
            y = y + dsk_s[l, :, cols] * x
            z = zd_buf[:, 128 + 128 * p:256 + 128 * p]
            v = y * (z * jax.nn.sigmoid(z))
            v_buf[:, cols] = v
            sq = sq + v * v
        return sq

    first_pairs = (n_pairs + 1) // 2

    def scan_a(j):
        sq_s[...] = scan_pairs(j, range(first_pairs))

    def scan_b(j):
        l, _ = split_item(j)
        sq = sq_s[...] + scan_pairs(j, range(first_pairs, n_pairs))
        ones = jnp.ones((8, 128), F32)
        part = lax.dot_general(ones, sq, (((1,), (1,)), ((), ())), precision=HI, preferred_element_type=F32)
        stats[j, 0:1, :] = part[0:1, :]
        for r in range(len(relations)):
            stat_copy(r, j).start()
        own = lax.rsqrt(jnp.sum(sq, axis=1, keepdims=True) * (1.0 / width) + EPS)
        for p in range(n_pairs):
            cols = slice(128 * p, 128 * (p + 1))
            g_buf[:, cols] = (v_buf[:, cols] * own * gate_s[l, :, cols]).astype(BF16)

    def out_proj(j, h):
        l, c = split_item(j)
        if h == 0:
            @pl.when(c == 0)
            def _():
                out_weight_copy(l).wait()

        g = g_buf[...]
        for n in range(h * half, (h + 1) * half, 256):
            p_buf[:, n:n + 256] = jnp.dot(g, w_o[l, :, n:n + 256], preferred_element_type=F32)
        rdma(0, j, h).start()

    def factors(j):
        wait_stats(j)
        st = stats[j]
        rs = lax.rsqrt(jnp.sum(st, axis=0, keepdims=True) * (1.0 / inner_width) + EPS)
        for k in range(2):
            own = lax.rsqrt(st[k:k + 1, :] * (1.0 / width) + EPS)
            f = rs / jnp.maximum(own, 1e-30)
            f_s[k] = jnp.broadcast_to(f, (T, T)).T

    def ev1(j, h, first):
        _, c = split_item(j)
        if first:
            factors(j)
        mine = core * (T // 2)
        rdma(0, j, h).wait()

        def add(off):
            f_me = f_s[0, at(mine + off, 16), :]
            f_peer = f_s[1, at(mine + off, 16), :]
            for n in range(h * half, (h + 1) * half, 128):
                cols = slice(n, n + 128)
                r0[c, at(off, 16), cols] = r0[c, at(off, 16), cols] * f_peer + p_buf[at(mine + off, 16), cols] * f_me

        add((1 - xi) * 16)
        rdma(1, j, h).start()
        add(32 + (1 - yi) * 16)
        rdma(2, j, h).start()
        add(xi * 16)
        add(32 + yi * 16)

    def ev2(j, h, first):
        _, c = split_item(j)
        cols = halves[h]
        wait_pair(1, j, h)
        r1a[c, :, cols] += r0[c, at(xi * 16, 16), cols]
        rdma(3, j, h).start()
        r1b[c, :, cols] += r0[c, at(32 + yi * 16, 16), cols]
        rdma(4, j, h).start()

    def ev3(j, h, first):
        l, c = split_item(j)
        cols = halves[h]
        base = c * T + core * (T // 2)
        rows_a = at(base + xi * 16 + yi * 8, 8)
        rows_b = at(base + 32 + yi * 16 + xi * 8, 8)
        wait_pair(3, j, h)
        val = r2a[c, :, cols] + r1a[c, at(yi * 8, 8), cols]
        u_buf[slot_of(l + 1), rows_a, cols] = (u_buf[slot_of(l), rows_a, cols] + val).astype(BF16).astype(F32)
        rdma(5, j, h).start()
        val = r2b[c, :, cols] + r1b[c, at(xi * 8, 8), cols]
        u_buf[slot_of(l + 1), rows_b, cols] = (u_buf[slot_of(l), rows_b, cols] + val).astype(BF16).astype(F32)
        rdma(6, j, h).start()

    def ev4(j, h, first):
        wait_pair(5, j, h)
        rdma(7, j, h).start()
        rdma(8, j, h).start()

    def ev5(j, h, first):
        wait_pair(7, j, h)
        rdma(9, j, h).start()

    def ev6(j, h, first):
        l, c = split_item(j)
        rdma(9, j, h).wait()

        def finish():
            @pl.loop(0, T // 16)
            def _(i):
                rows = at(c * T + i * 16, 16, 16)
                out_ref[0, rows, halves[h]] = u_buf[n_layers % 2, rows, halves[h]].astype(BF16)

        if isinstance(j, int):
            if l == n_layers - 1:
                finish()
        else:
            pl.when(l == n_layers - 1)(finish)

    steps = {1: ev1, 2: ev2, 3: ev3, 4: ev4, 5: ev5, 6: ev6}

    def run_step(step, item, h, first):
        with jax.named_scope("ev%d%d" % (step, h)):
            steps[step](item, h, first)

    def slot(k, j):
        for step, h, delta, first, only, skip in SLOTS[k]:
            if only:
                for item in only:
                    pl.when(j == item + delta)(functools.partial(run_step, step, item, h, first))
            else:
                item = j - delta
                there = jnp.logical_and(item >= 0, item < n_items)
                for other in skip:
                    there = jnp.logical_and(there, item != other)
                pl.when(there)(functools.partial(run_step, step, item, h, first))

    pl.semaphore_wait(barrier, len(relations))

    pieces = (in_norm, in_conv, in_gate, scan_prep, scan_a, scan_b, functools.partial(out_proj, h=0),
              functools.partial(out_proj, h=1))
    names = ("norm", "conv", "gate", "prep", "scan_a", "scan_b", "out0", "out1")

    @pl.loop(0, n_items)
    def _(j):
        for k, (piece, name) in enumerate(zip(pieces, names)):
            slot(k, j)

            @pl.when(jnp.logical_and(j >= 0, j < n_items))
            def _():
                with jax.named_scope(name):
                    piece(j)

        slot(len(pieces), j)

    for step, h, item, first in DRAIN:
        run_step(step, item, h, first)


def solution(mesh):
    tp_size = mesh.shape['tp']
    rep_spec = P()
    col_spec = P(None, None, 'tp')
    vec_spec = P(None, 'tp')
    in_specs = (P('dp'), rep_spec, col_spec, col_spec, rep_spec, col_spec, col_spec, rep_spec, vec_spec, rep_spec,
                vec_spec, vec_spec, vec_spec, vec_spec, P(None, 'tp', None))

    def device_forward(hidden, norm_w, w_z, w_x, w_bc, w_dt, conv_x, conv_bc, bias_x, bias_bc, dt_bias, a_log,
                       d_skip, gate_w, w_out):
        n_layers, d_model = norm_w.shape
        n_tok = hidden.shape[1]
        width = w_x.shape[-1]
        n_heads = dt_bias.shape[-1]
        conv_w = width + 2 * STATE
        n_chunks = n_tok // T
        n_items = n_layers * n_chunks
        any_spec = pl.BlockSpec(memory_space=pltpu.HBM)
        vmem_spec = pl.BlockSpec(memory_space=pltpu.VMEM)
        dma = pltpu.SemaphoreType.DMA
        return pl.pallas_call(
            functools.partial(mixer_kernel, n_layers, n_chunks, width * tp_size),
            out_shape=jax.ShapeDtypeStruct(hidden.shape, BF16),
            in_specs=[any_spec] * 15,
            out_specs=vmem_spec,
            scratch_shapes=[
                pltpu.VMEM(norm_w.shape, BF16),
                pltpu.VMEM(conv_x.shape, BF16),
                pltpu.VMEM(conv_bc.shape, BF16),
                pltpu.VMEM(bias_x.shape, BF16),
                pltpu.VMEM(bias_bc.shape, BF16),
                pltpu.VMEM(dt_bias.shape, F32),
                pltpu.VMEM(a_log.shape, F32),
                pltpu.VMEM(d_skip.shape, F32),
                pltpu.VMEM(gate_w.shape, BF16),
                pltpu.VMEM((n_layers, d_model, conv_w + 128 + width), BF16),
                pltpu.VMEM((n_layers, width, d_model), BF16),
                pltpu.VMEM((n_heads, n_layers, d_model), BF16),
                pltpu.VMEM((16 * n_layers, d_model), F32),
                pltpu.VMEM((n_tok, d_model), BF16),
                pltpu.VMEM((2, n_tok, d_model), F32),
                pltpu.VMEM((T, d_model), F32),
                pltpu.VMEM((n_chunks, T // 2, d_model), F32),
                pltpu.VMEM((n_chunks, 16, d_model), F32),
                pltpu.VMEM((n_chunks, 16, d_model), F32),
                pltpu.VMEM((n_chunks, 8, d_model), F32),
                pltpu.VMEM((n_chunks, 8, d_model), F32),
                pltpu.VMEM((T, d_model), BF16),
                pltpu.VMEM((T + 8, conv_w), F32),
                pltpu.VMEM((T, 128 + width), F32),
                pltpu.VMEM((T, width), F32),
                pltpu.VMEM((T, width), F32),
                pltpu.VMEM((T, width), BF16),
                pltpu.VMEM((STATE, width), F32),
                pltpu.VMEM((T, width), F32),
                pltpu.VMEM((T, 128), F32),
                pltpu.VMEM((128, T), F32),
                pltpu.VMEM((T, 128), F32),
                pltpu.VMEM((T, T), F32),
                pltpu.VMEM((STATE, T), F32),
                pltpu.VMEM((T, 128), F32),
                pltpu.VMEM((2, T, T), F32),
                pltpu.VMEM((n_items, 8, T), F32),
                pltpu.VMEM((n_layers, 1, d_model), F32),
                pltpu.VMEM((n_layers, 4, conv_w), F32),
                pltpu.VMEM((n_layers, 1, conv_w), F32),
                pltpu.VMEM((n_layers, 1, 128), F32),
                pltpu.VMEM((n_layers, 1, 128), F32),
                pltpu.VMEM((n_layers, 1, width), F32),
                pltpu.VMEM((n_layers, 1, width), F32),
                dma((n_layers, 3)),
                dma((3,)),
                dma((9,)),
                dma((n_chunks, 2, 6)),
                dma((n_chunks, 2, 6)),
                dma((n_chunks,)),
                dma((n_chunks,)),
            ],
            compiler_params=pltpu.CompilerParams(
                collective_id=0, has_side_effects=True, vmem_limit_bytes=50000000),
            name="mixer",
        )(*[pltpu.with_memory_space_constraint(arg, pltpu.HBM) for arg in (
            hidden, norm_w, w_z, w_x, w_bc, jnp.transpose(w_dt, (2, 0, 1)), conv_x, conv_bc, bias_x, bias_bc, dt_bias,
            a_log, d_skip, gate_w, w_out)])

    return jax.shard_map(device_forward, mesh=mesh, in_specs=in_specs, out_specs=P('dp'), check_vma=False)
```

```python
import functools

import jax
import jax.numpy as jnp
from jax import lax
from jax.experimental import pallas as pl
from jax.experimental.pallas import tpu as pltpu
from jax.sharding import PartitionSpec as P

EPS = 1e-5
T = 128
HEAD = 64
STATE = 64
HI = lax.Precision.HIGHEST
F32 = jnp.float32
BF16 = jnp.bfloat16

SLOTS = (
    ((4, 0, 3, 0, (), ()), (3, 1, 2, 0, (1,), ()), (1, 1, 1, 1, (1,), ()),),
    ((2, 1, 2, 0, (2,), ()), (1, 0, 1, 1, (), (0, 1, 2)), (1, 0, 1, 0, (), (0, 2, 3, 4, 5, 6)), (5, 0, 3, 0, (1,), ()), (1, 1, 1, 0, (), (0, 1, 2)),),
    ((3, 1, 2, 0, (), (0, 1, 2)), (1, 0, 1, 1, (2,), ()), (3, 0, 2, 0, (0,), ()), (1, 1, 1, 1, (0,), ()),),
    ((5, 1, 3, 0, (2,), ()),),
    ((1, 0, 1, 0, (0,), ()), (5, 1, 3, 0, (), (0, 2)), (6, 1, 3, 0, (), (0, 1)), (5, 0, 3, 0, (2,), ()), (3, 1, 2, 0, (2,), ()), (3, 0, 2, 0, (), (0,)), (5, 1, 3, 0, (0,), ()),),
    ((6, 0, 3, 0, (1,), ()), (1, 1, 1, 0, (2,), ()), (5, 0, 3, 0, (0,), ()), (2, 0, 1, 0, (), (0, 1)),),
    ((2, 1, 1, 0, (), (1, 2)), (5, 0, 3, 0, (), (0, 1, 2)), (6, 1, 3, 0, (1,), ()), (4, 1, 2, 0, (), (0, 2)), (2, 0, 1, 0, (1,), ()),),
    ((6, 0, 3, 0, (0,), ()), (6, 0, 3, 0, (), (0, 1, 2)), (2, 1, 1, 0, (1,), ()),),
    ((2, 0, 1, 0, (0,), ()), (4, 1, 2, 0, (0,), ()), (4, 1, 2, 0, (2,), ()), (6, 1, 3, 0, (0,), ()), (6, 0, 3, 0, (2,), ()), (3, 1, 1, 0, (0,), ()),),
)
DRAIN = ((4, 0, 5, 0), (1, 1, 7, 1), (5, 1, 5, 0), (1, 0, 7, 0), (2, 1, 7, 0), (3, 0, 6, 0), (3, 1, 6, 0), (5, 0, 5, 0), (2, 0, 7, 0), (3, 1, 7, 0), (4, 0, 6, 0), (3, 0, 7, 0), (6, 1, 5, 0), (4, 1, 6, 0), (5, 0, 6, 0), (4, 1, 7, 0), (4, 0, 7, 0), (6, 0, 6, 0), (5, 1, 6, 0), (5, 1, 7, 0), (5, 0, 7, 0), (6, 1, 6, 0), (6, 0, 5, 0), (6, 1, 7, 0), (6, 0, 7, 0))


def mixer_kernel(n_layers, n_chunks, inner_width,
                 hid_ref, norm_hbm, wz_ref, wx_ref, wbc_ref, wdt_ref, convx_hbm, convbc_hbm, biasx_hbm,
                 biasbc_hbm, dtb_hbm, alog_hbm, dskip_hbm, gate_hbm, wout_ref,
                 out_ref,
                 norm_ref, convx_ref, convbc_ref, biasx_ref, biasbc_ref, dtb_ref, alog_ref, dskip_ref, gate_ref,
                 w_in, w_o, wdt_s, wdt_f, hid_s, u_buf, p_buf, r0, r1a, r1b, r2a, r2b, h_buf, c_buf, zd_buf,
                 x_act, v_buf, g_buf, s_buf, cs_buf, acum_s, acumt_s, dt_s, g_s, bt_s, sq_s, f_s, stats,
                 norm_s, cw_s, cb_s, dtb_s, nega_s, dsk_s, gate_s,
                 w_sem, h_sem, par_sem, send_sem, recv_sem, st_send, st_recv):
    d_model = u_buf.shape[2]
    half = d_model // 2
    width = x_act.shape[1]
    n_pairs = width // (2 * HEAD)
    n_heads = dtb_ref.shape[1]
    conv_w = width + 2 * STATE
    n_items = n_layers * n_chunks

    me = lax.axis_index("tp")
    core = lax.rem(me, 2)
    xi = lax.rem(me // 2, 2)
    yi = me // 4

    def peer_id(dx, dy, dc):
        px = xi if dx == 0 else 1 - xi
        py = yi if dy == 0 else 1 - yi
        pc = core if dc == 0 else 1 - core
        return {"tp": py * 4 + px * 2 + pc}

    relations = [(dx, dy, dc) for dx in (0, 1) for dy in (0, 1) for dc in (0, 1)][1:]
    core_peer, x_peer, y_peer = peer_id(0, 0, 1), peer_id(1, 0, 0), peer_id(0, 1, 0)

    def split_item(j):
        if isinstance(j, int):
            return j // n_chunks, j % n_chunks
        return j // n_chunks, lax.rem(j, n_chunks)

    def slot_of(l):
        return l % 2 if isinstance(l, int) else lax.rem(l, 2)

    halves = [slice(0, half), slice(half, d_model)]

    def at(off, size, unit=8):
        return pl.ds(pl.multiple_of(off, unit), size)

    def conv_weight_copies(l):
        return [
            pltpu.make_async_copy(wx_ref.at[l], w_in.at[l, :, pl.ds(0, width)], w_sem.at[l, 0]),
            pltpu.make_async_copy(wbc_ref.at[l], w_in.at[l, :, pl.ds(width, 2 * STATE)], w_sem.at[l, 0]),
        ]

    def gate_weight_copy(l):
        return pltpu.make_async_copy(wz_ref.at[l], w_in.at[l, :, pl.ds(conv_w + 128, width)], w_sem.at[l, 1])

    def out_weight_copy(l):
        return pltpu.make_async_copy(wout_ref.at[l], w_o.at[l], w_sem.at[l, 2])

    def dt_weight_copy():
        return pltpu.make_async_copy(wdt_ref, wdt_s, h_sem.at[2])

    def hid_copy(k):
        rows = pl.ds(0, T) if k == 0 else pl.ds(T, (n_chunks - 1) * T)
        return pltpu.make_async_copy(hid_ref.at[0, rows, :], hid_s.at[rows, :], h_sem.at[k])

    def start_in_weights(l):
        for cp in conv_weight_copies(l):
            cp.start()
        gate_weight_copy(l).start()

    small = [pltpu.make_async_copy(src, dst, par_sem.at[i]) for i, (src, dst) in enumerate((
        (norm_hbm, norm_ref), (convx_hbm, convx_ref), (convbc_hbm, convbc_ref), (biasx_hbm, biasx_ref),
        (biasbc_hbm, biasbc_ref), (dtb_hbm, dtb_ref), (alog_hbm, alog_ref), (dskip_hbm, dskip_ref),
        (gate_hbm, gate_ref)))]

    small[0].start()
    hid_copy(0).start()
    dt_weight_copy().start()
    for cp in conv_weight_copies(0):
        cp.start()
    for cp in small[1:]:
        cp.start()

    barrier = pltpu.get_barrier_semaphore()
    for rel in relations:
        pl.semaphore_signal(barrier, inc=1, device_id=peer_id(*rel))

    lane = lax.broadcasted_iota(jnp.int32, (1, 128), 1)
    small[0].wait()
    gate_weight_copy(0).start()
    for l in range(n_layers):
        norm_s[l] = norm_ref[l:l + 1, :].astype(F32)

    def small_parameters():
        for cp in small[1:]:
            cp.wait()
        for l in range(n_layers):
            cw_s[l, :, 0:width] = convx_ref[l].astype(F32)
            cw_s[l, :, width:conv_w] = convbc_ref[l].astype(F32)
            cb_s[l, :, 0:width] = biasx_ref[l:l + 1, :].astype(F32)
            cb_s[l, :, width:conv_w] = biasbc_ref[l:l + 1, :].astype(F32)
            gate_s[l] = gate_ref[l:l + 1, :].astype(F32)
            dtb_s[l] = jnp.zeros((1, 128), F32)
            nega_s[l] = jnp.zeros((1, 128), F32)
            dtb_s[l, :, 0:n_heads] = dtb_ref[l:l + 1, :]
            nega_s[l, :, 0:n_heads] = -jnp.exp(alog_ref[l:l + 1, :])
            for p in range(n_pairs):
                d0 = dskip_ref[l:l + 1, 2 * p:2 * p + 1]
                d1 = dskip_ref[l:l + 1, 2 * p + 1:2 * p + 2]
                dsk_s[l, :, 128 * p:128 * (p + 1)] = jnp.where(lane < HEAD, d0, d1)

    def rdma(kind, j, h):
        l, c = split_item(j)
        cols = pl.ds(h * half, half)
        mine = core * (T // 2)
        base = c * T + mine
        group = (kind + 1) // 2
        if kind == 0:
            src, dst, dev = p_buf.at[at((1 - core) * (T // 2), T // 2), cols], r0.at[c, :, cols], core_peer
        elif kind == 1:
            src, dst, dev = r0.at[c, at((1 - xi) * 16, 16), cols], r1a.at[c, :, cols], x_peer
        elif kind == 2:
            src, dst, dev = r0.at[c, at(32 + (1 - yi) * 16, 16), cols], r1b.at[c, :, cols], y_peer
        elif kind == 3:
            src, dst, dev = r1a.at[c, at((1 - yi) * 8, 8), cols], r2a.at[c, :, cols], y_peer
        elif kind == 4:
            src, dst, dev = r1b.at[c, at((1 - xi) * 8, 8), cols], r2b.at[c, :, cols], x_peer
        else:
            off, size, dev = [
                (base + xi * 16 + yi * 8, 8, y_peer),
                (base + 32 + yi * 16 + xi * 8, 8, x_peer),
                (base + xi * 16, 16, x_peer),
                (base + 32 + yi * 16, 16, y_peer),
                (base, T // 2, core_peer),
            ][kind - 5]
            src = u_buf.at[slot_of(l + 1), at(off, size), cols]
            dst = src
        return pltpu.make_async_remote_copy(
            src_ref=src, dst_ref=dst, send_sem=send_sem.at[c, h, group], recv_sem=recv_sem.at[c, h, group],
            device_id=dev, device_id_type=pl.DeviceIdType.MESH)

    def wait_pair(kind, j, h):
        _, c = split_item(j)
        group = (kind + 1) // 2
        size = 32 if kind in (1, 7) else 16
        both = r0.at[c, pl.ds(0, size), pl.ds(h * half, half)]
        pltpu.make_async_copy(both, both, send_sem.at[c, h, group]).wait()
        pltpu.make_async_copy(both, both, recv_sem.at[c, h, group]).wait()

    def stat_copy(r, j):
        _, c = split_item(j)
        return pltpu.make_async_remote_copy(
            src_ref=stats.at[j, pl.ds(0, 1), :], dst_ref=stats.at[j, pl.ds(r + 1, 1), :],
            send_sem=st_send.at[c], recv_sem=st_recv.at[c],
            device_id=peer_id(*relations[r]), device_id_type=pl.DeviceIdType.MESH)

    def wait_stats(j):
        _, c = split_item(j)
        rows = stats.at[j, pl.ds(1, len(relations)), :]
        pltpu.make_async_copy(rows, rows, st_send.at[c]).wait()
        pltpu.make_async_copy(rows, rows, st_recv.at[c]).wait()

    def in_norm(j):
        l, c = split_item(j)
        base = c * T

        @pl.when(j == 0)
        def _():
            hid_copy(0).wait()

        @pl.when(j == 1)
        def _():
            hid_copy(1).wait()
            for k in range(1, n_layers):
                start_in_weights(k)
                out_weight_copy(k).start()

        def squares(load):
            @pl.loop(0, T // 16)
            def _(i):
                acc = jnp.zeros((16, 128), F32)
                for n in range(0, d_model, 128):
                    u = load(base + i * 16, slice(n, n + 128))
                    acc = acc + u * u
                sq_s[at(i * 16, 16, 16), :] = acc

        def load_hidden(off, cols):
            u = hid_s[at(off, 16, 16), cols].astype(F32)
            u_buf[0, at(off, 16, 16), cols] = u
            return u

        def load_u(off, cols):
            return u_buf[slot_of(l), at(off, 16, 16), cols]

        pl.when(l == 0)(lambda: squares(load_hidden))
        pl.when(l > 0)(lambda: squares(load_u))
        ms = jnp.sum(sq_s[...], axis=-1, keepdims=True) * (1.0 / d_model)
        sq_s[...] = jnp.broadcast_to(lax.rsqrt(ms + EPS), (T, 128))

        @pl.loop(0, T // 16)
        def _(i):
            rs = sq_s[at(i * 16, 16, 16), :]
            for n in range(0, d_model, 128):
                cols = slice(n, n + 128)
                h = load_u(base + i * 16, cols) * rs * norm_s[l, :, cols]
                h_buf[at(i * 16, 16, 16), cols] = h.astype(BF16)

        @pl.when(c == 0)
        def _():
            c_buf[0:8, :] = jnp.zeros((8, conv_w), F32)
            s_buf[...] = jnp.zeros_like(s_buf)

        @pl.when(c > 0)
        def _():
            c_buf[0:8, :] = c_buf[T:T + 8, :]

    def in_conv(j):
        l, c = split_item(j)

        @pl.when(j == 0)
        def _():
            small_parameters()
            dt_weight_copy().wait()
            for k in range(n_layers):
                wdt_f[16 * k + 8:16 * k + 16, :] = jnp.zeros((8, d_model), F32)
            for n in range(n_heads):
                rows = wdt_s[n].astype(F32)
                for k in range(n_layers):
                    wdt_f[16 * k + n:16 * k + n + 1, :] = rows[k:k + 1, :]

        @pl.when(c == 0)
        def _():
            both = w_in.at[l, :, pl.ds(0, conv_w)]
            pltpu.make_async_copy(both, both, w_sem.at[l, 0]).wait()

        h = h_buf[...]
        for n in range(0, conv_w, 256):
            r = jnp.dot(h, w_in[l, :, n:n + 256], preferred_element_type=F32)
            c_buf[8:8 + T, n:n + 256] = r.astype(BF16).astype(F32)

    def in_gate(j):
        l, c = split_item(j)

        @pl.when(c == 0)
        def _():
            w_in[l, :, conv_w:conv_w + 128] = jnp.zeros((d_model, 128), BF16)
            w_in[l, :, conv_w:conv_w + 16] = wdt_f[at(16 * l, 16), :].T.astype(BF16)
            gate_weight_copy(l).wait()

        @pl.when(j == 0)
        def _():
            out_weight_copy(0).start()
            hid_copy(1).start()

        h = h_buf[...]
        for n in range(0, width + 128, 256):
            r = jnp.dot(h, w_in[l, :, conv_w + n:conv_w + n + 256], preferred_element_type=F32)
            zd_buf[:, n:n + 256] = r.astype(BF16).astype(F32)

    def scan_prep(j):
        l, _ = split_item(j)
        b_act = None
        for n in range(0, conv_w, 128):
            cols = slice(n, n + 128)
            acc = cb_s[l, :, cols] + c_buf[5:5 + T, cols] * cw_s[l, 0:1, cols]
            for k in range(1, 4):
                acc = acc + c_buf[5 + k:5 + k + T, cols] * cw_s[l, k:k + 1, cols]
            act = acc * jax.nn.sigmoid(acc)
            if n < width:
                x_act[:, cols] = act
            else:
                b_act = act
        bt = b_act.T[0:STATE, :]
        c_mat = b_act[:, STATE:2 * STATE]
        bt_s[...] = bt
        g_s[...] = jnp.dot(c_mat, bt, precision=HI, preferred_element_type=F32)
        cs_buf[...] = jnp.dot(c_mat, s_buf[...], precision=HI, preferred_element_type=F32)
        dt = jax.nn.softplus(zd_buf[:, 0:128] + dtb_s[l])
        a = dt * nega_s[l]
        row = lax.broadcasted_iota(jnp.int32, (T, T), 0)
        col = lax.broadcasted_iota(jnp.int32, (T, T), 1)
        tril = jnp.where(row >= col, 1.0, 0.0).astype(F32)
        acum = jnp.dot(tril, a, precision=HI, preferred_element_type=F32)
        dt_s[...] = dt
        acum_s[...] = acum
        acumt_s[...] = acum.T

    def scan_pairs(j, pairs):
        l, _ = split_item(j)
        row = lax.broadcasted_iota(jnp.int32, (T, T), 0)
        col = lax.broadcasted_iota(jnp.int32, (T, T), 1)
        causal = row >= col
        low = col < HEAD
        low_row = lane < HEAD
        g = g_s[...]
        bt = bt_s[...]
        sq = jnp.zeros((T, 128), F32)
        for p in pairs:
            h0, h1 = 2 * p, 2 * p + 1
            cols = slice(128 * p, 128 * (p + 1))
            a0 = jnp.broadcast_to(acum_s[:, h0:h0 + 1], (T, T))
            a1 = jnp.broadcast_to(acum_s[:, h1:h1 + 1], (T, T))
            m0 = jnp.where(causal, jnp.exp(jnp.minimum(a0 - acumt_s[h0:h0 + 1, :], 0.0)), 0.0) * g
            m1 = jnp.where(causal, jnp.exp(jnp.minimum(a1 - acumt_s[h1:h1 + 1, :], 0.0)), 0.0) * g
            dt = jnp.where(low, dt_s[:, h0:h0 + 1], dt_s[:, h1:h1 + 1])
            x = x_act[:, cols]
            xd = x * dt
            both = jnp.concatenate([m0, m1], axis=1)
            split = jnp.concatenate([jnp.where(low, xd, 0.0), jnp.where(low, 0.0, xd)], axis=0)
            y = jnp.dot(both, split, precision=HI, preferred_element_type=F32)
            ap = jnp.where(low, a0, a1)
            last = jnp.where(low_row, acum_s[T - 1:T, h0:h0 + 1], acum_s[T - 1:T, h1:h1 + 1])
            y = y + cs_buf[:, cols] * jnp.exp(ap)
            xt = xd * jnp.exp(last - ap)
            s_buf[:, cols] = s_buf[:, cols] * jnp.exp(last) + jnp.dot(bt, xt, precision=HI, preferred_element_type=F32)
            y = y + dsk_s[l, :, cols] * x
            z = zd_buf[:, 128 + 128 * p:256 + 128 * p]
            v = y * (z * jax.nn.sigmoid(z))
            v_buf[:, cols] = v
            sq = sq + v * v
        return sq

    first_pairs = (n_pairs + 1) // 2

    def scan_a(j):
        sq_s[...] = scan_pairs(j, range(first_pairs))

    def scan_b(j):
        l, _ = split_item(j)
        sq = sq_s[...] + scan_pairs(j, range(first_pairs, n_pairs))
        ones = jnp.ones((8, 128), F32)
        part = lax.dot_general(ones, sq, (((1,), (1,)), ((), ())), precision=HI, preferred_element_type=F32)
        stats[j, 0:1, :] = part[0:1, :]
        for r in range(len(relations)):
            stat_copy(r, j).start()
        own = lax.rsqrt(jnp.sum(sq, axis=1, keepdims=True) * (1.0 / width) + EPS)
        for p in range(n_pairs):
            cols = slice(128 * p, 128 * (p + 1))
            g_buf[:, cols] = (v_buf[:, cols] * own * gate_s[l, :, cols]).astype(BF16)

    def out_proj(j, h):
        l, c = split_item(j)
        if h == 0:
            @pl.when(c == 0)
            def _():
                out_weight_copy(l).wait()

        g = g_buf[...]
        for n in range(h * half, (h + 1) * half, 256):
            p_buf[:, n:n + 256] = jnp.dot(g, w_o[l, :, n:n + 256], preferred_element_type=F32)
        rdma(0, j, h).start()

    def factors(j):
        wait_stats(j)
        st = stats[j]
        rs = lax.rsqrt(jnp.sum(st, axis=0, keepdims=True) * (1.0 / inner_width) + EPS)
        for k in range(2):
            own = lax.rsqrt(st[k:k + 1, :] * (1.0 / width) + EPS)
            f = rs / jnp.maximum(own, 1e-30)
            f_s[k] = jnp.broadcast_to(f, (T, T)).T

    def ev1(j, h, first):
        _, c = split_item(j)
        if first:
            factors(j)
        mine = core * (T // 2)
        rdma(0, j, h).wait()

        def add(off):
            f_me = f_s[0, at(mine + off, 16), :]
            f_peer = f_s[1, at(mine + off, 16), :]
            for n in range(h * half, (h + 1) * half, 128):
                cols = slice(n, n + 128)
                r0[c, at(off, 16), cols] = r0[c, at(off, 16), cols] * f_peer + p_buf[at(mine + off, 16), cols] * f_me

        add((1 - xi) * 16)
        rdma(1, j, h).start()
        add(32 + (1 - yi) * 16)
        rdma(2, j, h).start()
        add(xi * 16)
        add(32 + yi * 16)

    def ev2(j, h, first):
        _, c = split_item(j)
        cols = halves[h]
        wait_pair(1, j, h)
        r1a[c, :, cols] += r0[c, at(xi * 16, 16), cols]
        rdma(3, j, h).start()
        r1b[c, :, cols] += r0[c, at(32 + yi * 16, 16), cols]
        rdma(4, j, h).start()

    def ev3(j, h, first):
        l, c = split_item(j)
        cols = halves[h]
        base = c * T + core * (T // 2)
        rows_a = at(base + xi * 16 + yi * 8, 8)
        rows_b = at(base + 32 + yi * 16 + xi * 8, 8)
        wait_pair(3, j, h)
        val = r2a[c, :, cols] + r1a[c, at(yi * 8, 8), cols]
        u_buf[slot_of(l + 1), rows_a, cols] = (u_buf[slot_of(l), rows_a, cols] + val).astype(BF16).astype(F32)
        rdma(5, j, h).start()
        val = r2b[c, :, cols] + r1b[c, at(xi * 8, 8), cols]
        u_buf[slot_of(l + 1), rows_b, cols] = (u_buf[slot_of(l), rows_b, cols] + val).astype(BF16).astype(F32)
        rdma(6, j, h).start()

    def ev4(j, h, first):
        wait_pair(5, j, h)
        rdma(7, j, h).start()
        rdma(8, j, h).start()

    def ev5(j, h, first):
        wait_pair(7, j, h)
        rdma(9, j, h).start()

    def ev6(j, h, first):
        l, c = split_item(j)
        rdma(9, j, h).wait()

        def finish():
            @pl.loop(0, T // 16)
            def _(i):
                rows = at(c * T + i * 16, 16, 16)
                out_ref[0, rows, halves[h]] = u_buf[n_layers % 2, rows, halves[h]].astype(BF16)

        if isinstance(j, int):
            if l == n_layers - 1:
                finish()
        else:
            pl.when(l == n_layers - 1)(finish)

    steps = {1: ev1, 2: ev2, 3: ev3, 4: ev4, 5: ev5, 6: ev6}

    def run_step(step, item, h, first):
        with jax.named_scope("ev%d%d" % (step, h)):
            steps[step](item, h, first)

    def slot(k, j):
        for step, h, delta, first, only, skip in SLOTS[k]:
            if only:
                for item in only:
                    pl.when(j == item + delta)(functools.partial(run_step, step, item, h, first))
            else:
                item = j - delta
                there = jnp.logical_and(item >= 0, item < n_items)
                for other in skip:
                    there = jnp.logical_and(there, item != other)
                pl.when(there)(functools.partial(run_step, step, item, h, first))

    pl.semaphore_wait(barrier, len(relations))

    pieces = (in_norm, in_conv, in_gate, scan_prep, scan_a, scan_b, functools.partial(out_proj, h=0),
              functools.partial(out_proj, h=1))
    names = ("norm", "conv", "gate", "prep", "scan_a", "scan_b", "out0", "out1")

    @pl.loop(0, n_items)
    def _(j):
        for k, (piece, name) in enumerate(zip(pieces, names)):
            slot(k, j)

            @pl.when(jnp.logical_and(j >= 0, j < n_items))
            def _():
                with jax.named_scope(name):
                    piece(j)

        slot(len(pieces), j)

    for step, h, item, first in DRAIN:
        run_step(step, item, h, first)


def solution(mesh):
    tp_size = mesh.shape['tp']
    rep_spec = P()
    col_spec = P(None, None, 'tp')
    vec_spec = P(None, 'tp')
    in_specs = (P('dp'), rep_spec, col_spec, col_spec, rep_spec, col_spec, col_spec, rep_spec, vec_spec, rep_spec,
                vec_spec, vec_spec, vec_spec, vec_spec, P(None, 'tp', None))

    def device_forward(hidden, norm_w, w_z, w_x, w_bc, w_dt, conv_x, conv_bc, bias_x, bias_bc, dt_bias, a_log,
                       d_skip, gate_w, w_out):
        n_layers, d_model = norm_w.shape
        n_tok = hidden.shape[1]
        width = w_x.shape[-1]
        n_heads = dt_bias.shape[-1]
        conv_w = width + 2 * STATE
        n_chunks = n_tok // T
        n_items = n_layers * n_chunks
        any_spec = pl.BlockSpec(memory_space=pltpu.HBM)
        vmem_spec = pl.BlockSpec(memory_space=pltpu.VMEM)
        dma = pltpu.SemaphoreType.DMA
        return pl.pallas_call(
            functools.partial(mixer_kernel, n_layers, n_chunks, width * tp_size),
            out_shape=jax.ShapeDtypeStruct(hidden.shape, BF16),
            in_specs=[any_spec] * 15,
            out_specs=vmem_spec,
            scratch_shapes=[
                pltpu.VMEM(norm_w.shape, BF16),
                pltpu.VMEM(conv_x.shape, BF16),
                pltpu.VMEM(conv_bc.shape, BF16),
                pltpu.VMEM(bias_x.shape, BF16),
                pltpu.VMEM(bias_bc.shape, BF16),
                pltpu.VMEM(dt_bias.shape, F32),
                pltpu.VMEM(a_log.shape, F32),
                pltpu.VMEM(d_skip.shape, F32),
                pltpu.VMEM(gate_w.shape, BF16),
                pltpu.VMEM((n_layers, d_model, conv_w + 128 + width), BF16),
                pltpu.VMEM((n_layers, width, d_model), BF16),
                pltpu.VMEM((n_heads, n_layers, d_model), BF16),
                pltpu.VMEM((16 * n_layers, d_model), F32),
                pltpu.VMEM((n_tok, d_model), BF16),
                pltpu.VMEM((2, n_tok, d_model), F32),
                pltpu.VMEM((T, d_model), F32),
                pltpu.VMEM((n_chunks, T // 2, d_model), F32),
                pltpu.VMEM((n_chunks, 16, d_model), F32),
                pltpu.VMEM((n_chunks, 16, d_model), F32),
                pltpu.VMEM((n_chunks, 8, d_model), F32),
                pltpu.VMEM((n_chunks, 8, d_model), F32),
                pltpu.VMEM((T, d_model), BF16),
                pltpu.VMEM((T + 8, conv_w), F32),
                pltpu.VMEM((T, 128 + width), F32),
                pltpu.VMEM((T, width), F32),
                pltpu.VMEM((T, width), F32),
                pltpu.VMEM((T, width), BF16),
                pltpu.VMEM((STATE, width), F32),
                pltpu.VMEM((T, width), F32),
                pltpu.VMEM((T, 128), F32),
                pltpu.VMEM((128, T), F32),
                pltpu.VMEM((T, 128), F32),
                pltpu.VMEM((T, T), F32),
                pltpu.VMEM((STATE, T), F32),
                pltpu.VMEM((T, 128), F32),
                pltpu.VMEM((2, T, T), F32),
                pltpu.VMEM((n_items, 8, T), F32),
                pltpu.VMEM((n_layers, 1, d_model), F32),
                pltpu.VMEM((n_layers, 4, conv_w), F32),
                pltpu.VMEM((n_layers, 1, conv_w), F32),
                pltpu.VMEM((n_layers, 1, 128), F32),
                pltpu.VMEM((n_layers, 1, 128), F32),
                pltpu.VMEM((n_layers, 1, width), F32),
                pltpu.VMEM((n_layers, 1, width), F32),
                dma((n_layers, 3)),
                dma((3,)),
                dma((9,)),
                dma((n_chunks, 2, 6)),
                dma((n_chunks, 2, 6)),
                dma((n_chunks,)),
                dma((n_chunks,)),
            ],
            compiler_params=pltpu.CompilerParams(
                collective_id=0, has_side_effects=True, vmem_limit_bytes=50000000),
            name="mixer",
        )(*[pltpu.with_memory_space_constraint(arg, pltpu.HBM) for arg in (
            hidden, norm_w, w_z, w_x, w_bc, jnp.transpose(w_dt, (2, 0, 1)), conv_x, conv_bc, bias_x, bias_bc, dt_bias,
            a_log, d_skip, gate_w, w_out)])

    return jax.shard_map(device_forward, mesh=mesh, in_specs=in_specs, out_specs=P('dp'), check_vma=False)
```

```python
import functools

import jax
import jax.numpy as jnp
from jax import lax
from jax.experimental import pallas as pl
from jax.experimental.pallas import tpu as pltpu
from jax.sharding import PartitionSpec as P

EPS = 1e-5
T = 128
HEAD = 64
STATE = 64
HI = lax.Precision.HIGHEST
F32 = jnp.float32
BF16 = jnp.bfloat16

SLOTS = (
    ((1, 0, 1, 1, (), (0, 1, 2)), (1, 1, 1, 0, (2,), ()),),
    ((1, 0, 1, 1, (0,), ()), (1, 0, 1, 1, (1,), ()),),
    ((5, 1, 3, 0, (0,), ()), (5, 0, 3, 0, (2,), ()), (3, 1, 2, 0, (2,), ()), (1, 1, 1, 0, (), (0, 1, 2)), (5, 0, 3, 0, (), (0, 1, 2)),),
    ((3, 0, 2, 0, (1,), ()), (3, 0, 2, 0, (0,), ()), (5, 1, 3, 0, (2,), ()), (5, 0, 3, 0, (0,), ()), (1, 1, 1, 0, (0,), ()), (3, 1, 2, 0, (1,), ()),),
    ((3, 1, 2, 0, (), (1, 2)), (5, 1, 3, 0, (), (0, 1, 2)), (1, 1, 1, 0, (1,), ()), (5, 0, 3, 0, (1,), ()), (2, 0, 1, 1, (), (0,)),),
    ((6, 0, 3, 0, (), (0, 2)), (2, 1, 1, 0, (2,), ()), (4, 1, 2, 0, (2,), ()), (4, 0, 2, 0, (), (1,)),),
    ((4, 1, 2, 0, (1,), ()), (6, 0, 3, 0, (2,), ()), (6, 1, 3, 0, (), (0, 1, 2)), (2, 0, 1, 1, (0,), ()), (5, 1, 3, 0, (1,), ()),),
    ((4, 0, 2, 0, (1,), ()), (2, 1, 1, 0, (1,), ()), (6, 0, 3, 0, (0,), ()), (2, 1, 1, 0, (), (1, 2)), (6, 1, 3, 0, (0,), ()), (4, 1, 2, 0, (), (0, 1, 2)), (3, 0, 1, 0, (), (0, 1, 2)), (4, 1, 2, 0, (0,), ()),),
    ((6, 1, 3, 0, (2,), ()), (6, 1, 3, 0, (1,), ()), (1, 0, 0, 1, (2,), ()), (3, 0, 1, 0, (2,), ()),),
)
DRAIN = ((1, 1, 7, 1), (5, 1, 5, 0), (1, 0, 7, 0), (2, 1, 7, 1), (3, 1, 6, 0), (5, 0, 5, 0), (2, 0, 7, 0), (3, 1, 7, 0), (4, 0, 6, 0), (3, 0, 7, 0), (6, 1, 5, 0), (4, 1, 6, 0), (5, 0, 6, 0), (4, 1, 7, 0), (4, 0, 7, 0), (6, 0, 6, 0), (5, 1, 6, 0), (5, 1, 7, 0), (5, 0, 7, 0), (6, 1, 6, 0), (6, 0, 5, 0), (6, 1, 7, 0), (6, 0, 7, 0))


def mixer_kernel(n_layers, n_chunks, inner_width,
                 hid_ref, norm_hbm, wz_ref, wx_ref, wbc_ref, wdt_ref, convx_hbm, convbc_hbm, biasx_hbm,
                 biasbc_hbm, dtb_hbm, alog_hbm, dskip_hbm, gate_hbm, wout_ref,
                 out_ref,
                 norm_ref, convx_ref, convbc_ref, biasx_ref, biasbc_ref, dtb_ref, alog_ref, dskip_ref, gate_ref,
                 w_in, w_o, wdt_s, wdt_f, hid_s, u_buf, p_buf, r0, r1a, r1b, r2a, r2b, h_buf, c_buf, zd_buf,
                 x_act, v_buf, g_buf, s_buf, cs_buf, acum_s, acumt_s, dt_s, g_s, bt_s, sq_s, f_s, stats,
                 norm_s, cw_s, cb_s, dtb_s, nega_s, dsk_s, gate_s,
                 w_sem, h_sem, par_sem, send_sem, recv_sem, st_send, st_recv):
    d_model = u_buf.shape[2]
    half = d_model // 2
    width = x_act.shape[1]
    n_pairs = width // (2 * HEAD)
    n_heads = dtb_ref.shape[1]
    conv_w = width + 2 * STATE
    n_items = n_layers * n_chunks

    me = lax.axis_index("tp")
    core = lax.rem(me, 2)
    xi = lax.rem(me // 2, 2)
    yi = me // 4

    def peer_id(dx, dy, dc):
        px = xi if dx == 0 else 1 - xi
        py = yi if dy == 0 else 1 - yi
        pc = core if dc == 0 else 1 - core
        return {"tp": py * 4 + px * 2 + pc}

    relations = [(dx, dy, dc) for dx in (0, 1) for dy in (0, 1) for dc in (0, 1)][1:]
    core_peer, x_peer, y_peer = peer_id(0, 0, 1), peer_id(1, 0, 0), peer_id(0, 1, 0)

    def split_item(j):
        if isinstance(j, int):
            return j // n_chunks, j % n_chunks
        return j // n_chunks, lax.rem(j, n_chunks)

    def slot_of(l):
        return l % 2 if isinstance(l, int) else lax.rem(l, 2)

    halves = [slice(0, half), slice(half, d_model)]

    def at(off, size, unit=8):
        return pl.ds(pl.multiple_of(off, unit), size)

    def conv_weight_copies(l):
        return [
            pltpu.make_async_copy(wx_ref.at[l], w_in.at[l, :, pl.ds(0, width)], w_sem.at[l, 0]),
            pltpu.make_async_copy(wbc_ref.at[l], w_in.at[l, :, pl.ds(width, 2 * STATE)], w_sem.at[l, 0]),
        ]

    def gate_weight_copy(l):
        return pltpu.make_async_copy(wz_ref.at[l], w_in.at[l, :, pl.ds(conv_w + 128, width)], w_sem.at[l, 1])

    def out_weight_copy(l):
        return pltpu.make_async_copy(wout_ref.at[l], w_o.at[l], w_sem.at[l, 2])

    def dt_weight_copy():
        return pltpu.make_async_copy(wdt_ref, wdt_s, h_sem.at[2])

    def hid_copy(k):
        rows = pl.ds(0, T) if k == 0 else pl.ds(T, (n_chunks - 1) * T)
        return pltpu.make_async_copy(hid_ref.at[0, rows, :], hid_s.at[rows, :], h_sem.at[k])

    def start_in_weights(l):
        for cp in conv_weight_copies(l):
            cp.start()
        gate_weight_copy(l).start()

    small = [pltpu.make_async_copy(src, dst, par_sem.at[i]) for i, (src, dst) in enumerate((
        (norm_hbm, norm_ref), (convx_hbm, convx_ref), (convbc_hbm, convbc_ref), (biasx_hbm, biasx_ref),
        (biasbc_hbm, biasbc_ref), (dtb_hbm, dtb_ref), (alog_hbm, alog_ref), (dskip_hbm, dskip_ref),
        (gate_hbm, gate_ref)))]

    small[0].start()
    hid_copy(0).start()
    dt_weight_copy().start()
    for cp in conv_weight_copies(0):
        cp.start()
    for cp in small[1:]:
        cp.start()

    barrier = pltpu.get_barrier_semaphore()
    for rel in relations:
        pl.semaphore_signal(barrier, inc=1, device_id=peer_id(*rel))

    lane = lax.broadcasted_iota(jnp.int32, (1, 128), 1)
    small[0].wait()
    gate_weight_copy(0).start()
    for l in range(n_layers):
        norm_s[l] = norm_ref[l:l + 1, :].astype(F32)

    def small_parameters():
        for cp in small[1:]:
            cp.wait()
        for l in range(n_layers):
            cw_s[l, :, 0:width] = convx_ref[l].astype(F32)
            cw_s[l, :, width:conv_w] = convbc_ref[l].astype(F32)
            cb_s[l, :, 0:width] = biasx_ref[l:l + 1, :].astype(F32)
            cb_s[l, :, width:conv_w] = biasbc_ref[l:l + 1, :].astype(F32)
            gate_s[l] = gate_ref[l:l + 1, :].astype(F32)
            dtb_s[l] = jnp.zeros((1, 128), F32)
            nega_s[l] = jnp.zeros((1, 128), F32)
            dtb_s[l, :, 0:n_heads] = dtb_ref[l:l + 1, :]
            nega_s[l, :, 0:n_heads] = -jnp.exp(alog_ref[l:l + 1, :])
            for p in range(n_pairs):
                d0 = dskip_ref[l:l + 1, 2 * p:2 * p + 1]
                d1 = dskip_ref[l:l + 1, 2 * p + 1:2 * p + 2]
                dsk_s[l, :, 128 * p:128 * (p + 1)] = jnp.where(lane < HEAD, d0, d1)

    def rdma(kind, j, h):
        l, c = split_item(j)
        cols = pl.ds(h * half, half)
        mine = core * (T // 2)
        base = c * T + mine
        group = (kind + 1) // 2
        if kind == 0:
            src, dst, dev = p_buf.at[at((1 - core) * (T // 2), T // 2), cols], r0.at[c, :, cols], core_peer
        elif kind == 1:
            src, dst, dev = r0.at[c, at((1 - xi) * 16, 16), cols], r1a.at[c, :, cols], x_peer
        elif kind == 2:
            src, dst, dev = r0.at[c, at(32 + (1 - yi) * 16, 16), cols], r1b.at[c, :, cols], y_peer
        elif kind == 3:
            src, dst, dev = r1a.at[c, at((1 - yi) * 8, 8), cols], r2a.at[c, :, cols], y_peer
        elif kind == 4:
            src, dst, dev = r1b.at[c, at((1 - xi) * 8, 8), cols], r2b.at[c, :, cols], x_peer
        else:
            off, size, dev = [
                (base + xi * 16 + yi * 8, 8, y_peer),
                (base + 32 + yi * 16 + xi * 8, 8, x_peer),
                (base + xi * 16, 16, x_peer),
                (base + 32 + yi * 16, 16, y_peer),
                (base, T // 2, core_peer),
            ][kind - 5]
            src = u_buf.at[slot_of(l + 1), at(off, size), cols]
            dst = src
        return pltpu.make_async_remote_copy(
            src_ref=src, dst_ref=dst, send_sem=send_sem.at[c, h, group], recv_sem=recv_sem.at[c, h, group],
            device_id=dev, device_id_type=pl.DeviceIdType.MESH)

    def wait_pair(kind, j, h):
        _, c = split_item(j)
        group = (kind + 1) // 2
        size = 32 if kind in (1, 7) else 16
        both = r0.at[c, pl.ds(0, size), pl.ds(h * half, half)]
        pltpu.make_async_copy(both, both, send_sem.at[c, h, group]).wait()
        pltpu.make_async_copy(both, both, recv_sem.at[c, h, group]).wait()

    def stat_copy(r, j):
        _, c = split_item(j)
        return pltpu.make_async_remote_copy(
            src_ref=stats.at[j, pl.ds(0, 1), :], dst_ref=stats.at[j, pl.ds(r + 1, 1), :],
            send_sem=st_send.at[c, min(r, 1)], recv_sem=st_recv.at[c, min(r, 1)],
            device_id=peer_id(*relations[r]), device_id_type=pl.DeviceIdType.MESH)

    def wait_stats(j, k):
        _, c = split_item(j)
        rows = stats.at[j, pl.ds(1, 1) if k == 0 else pl.ds(2, len(relations) - 1), :]
        pltpu.make_async_copy(rows, rows, st_send.at[c, k]).wait()
        pltpu.make_async_copy(rows, rows, st_recv.at[c, k]).wait()

    def in_norm(j):
        l, c = split_item(j)
        base = c * T

        @pl.when(j == 0)
        def _():
            hid_copy(0).wait()

        @pl.when(j == 1)
        def _():
            hid_copy(1).wait()
            for k in range(1, n_layers):
                start_in_weights(k)
                out_weight_copy(k).start()

        def squares(load):
            @pl.loop(0, T // 16)
            def _(i):
                acc = jnp.zeros((16, 128), F32)
                for n in range(0, d_model, 128):
                    u = load(base + i * 16, slice(n, n + 128))
                    acc = acc + u * u
                sq_s[at(i * 16, 16, 16), :] = acc

        def load_hidden(off, cols):
            u = hid_s[at(off, 16, 16), cols].astype(F32)
            u_buf[0, at(off, 16, 16), cols] = u
            return u

        def load_u(off, cols):
            return u_buf[slot_of(l), at(off, 16, 16), cols]

        pl.when(l == 0)(lambda: squares(load_hidden))
        pl.when(l > 0)(lambda: squares(load_u))
        ms = jnp.sum(sq_s[...], axis=-1, keepdims=True) * (1.0 / d_model)
        sq_s[...] = jnp.broadcast_to(lax.rsqrt(ms + EPS), (T, 128))

        @pl.loop(0, T // 16)
        def _(i):
            rs = sq_s[at(i * 16, 16, 16), :]
            for n in range(0, d_model, 128):
                cols = slice(n, n + 128)
                h = load_u(base + i * 16, cols) * rs * norm_s[l, :, cols]
                h_buf[at(i * 16, 16, 16), cols] = h.astype(BF16)

        @pl.when(c == 0)
        def _():
            c_buf[0:8, :] = jnp.zeros((8, conv_w), F32)
            s_buf[...] = jnp.zeros_like(s_buf)

        @pl.when(c > 0)
        def _():
            c_buf[0:8, :] = c_buf[T:T + 8, :]

    def in_conv(j):
        l, c = split_item(j)

        @pl.when(j == 0)
        def _():
            small_parameters()
            dt_weight_copy().wait()
            for k in range(n_layers):
                wdt_f[16 * k + 8:16 * k + 16, :] = jnp.zeros((8, d_model), F32)
            for n in range(n_heads):
                rows = wdt_s[n].astype(F32)
                for k in range(n_layers):
                    wdt_f[16 * k + n:16 * k + n + 1, :] = rows[k:k + 1, :]

        @pl.when(c == 0)
        def _():
            both = w_in.at[l, :, pl.ds(0, conv_w)]
            pltpu.make_async_copy(both, both, w_sem.at[l, 0]).wait()

        h = h_buf[...]
        for n in range(0, conv_w, 256):
            r = jnp.dot(h, w_in[l, :, n:n + 256], preferred_element_type=F32)
            c_buf[8:8 + T, n:n + 256] = r.astype(BF16).astype(F32)

    def in_gate(j):
        l, c = split_item(j)

        @pl.when(c == 0)
        def _():
            w_in[l, :, conv_w:conv_w + 128] = jnp.zeros((d_model, 128), BF16)
            w_in[l, :, conv_w:conv_w + 16] = wdt_f[at(16 * l, 16), :].T.astype(BF16)
            gate_weight_copy(l).wait()

        @pl.when(j == 0)
        def _():
            out_weight_copy(0).start()
            hid_copy(1).start()

        h = h_buf[...]
        for n in range(0, width + 128, 256):
            r = jnp.dot(h, w_in[l, :, conv_w + n:conv_w + n + 256], preferred_element_type=F32)
            zd_buf[:, n:n + 256] = r.astype(BF16).astype(F32)

    def scan_prep(j):
        l, _ = split_item(j)
        b_act = None
        for n in range(0, conv_w, 128):
            cols = slice(n, n + 128)
            acc = cb_s[l, :, cols] + c_buf[5:5 + T, cols] * cw_s[l, 0:1, cols]
            for k in range(1, 4):
                acc = acc + c_buf[5 + k:5 + k + T, cols] * cw_s[l, k:k + 1, cols]
            act = acc * jax.nn.sigmoid(acc)
            if n < width:
                x_act[:, cols] = act
            else:
                b_act = act
        bt = b_act.T[0:STATE, :]
        c_mat = b_act[:, STATE:2 * STATE]
        bt_s[...] = bt
        g_s[...] = jnp.dot(c_mat, bt, precision=HI, preferred_element_type=F32)
        cs_buf[...] = jnp.dot(c_mat, s_buf[...], precision=HI, preferred_element_type=F32)
        dt = jax.nn.softplus(zd_buf[:, 0:128] + dtb_s[l])
        a = dt * nega_s[l]
        row = lax.broadcasted_iota(jnp.int32, (T, T), 0)
        col = lax.broadcasted_iota(jnp.int32, (T, T), 1)
        tril = jnp.where(row >= col, 1.0, 0.0).astype(F32)
        acum = jnp.dot(tril, a, precision=HI, preferred_element_type=F32)
        dt_s[...] = dt
        acum_s[...] = acum
        acumt_s[...] = acum.T

    def scan_pairs(j, pairs):
        l, _ = split_item(j)
        row = lax.broadcasted_iota(jnp.int32, (T, T), 0)
        col = lax.broadcasted_iota(jnp.int32, (T, T), 1)
        causal = row >= col
        low = col < HEAD
        low_row = lane < HEAD
        g = g_s[...]
        bt = bt_s[...]
        sq = jnp.zeros((T, 128), F32)
        for p in pairs:
            h0, h1 = 2 * p, 2 * p + 1
            cols = slice(128 * p, 128 * (p + 1))
            a0 = jnp.broadcast_to(acum_s[:, h0:h0 + 1], (T, T))
            a1 = jnp.broadcast_to(acum_s[:, h1:h1 + 1], (T, T))
            m0 = jnp.where(causal, jnp.exp(jnp.minimum(a0 - acumt_s[h0:h0 + 1, :], 0.0)), 0.0) * g
            m1 = jnp.where(causal, jnp.exp(jnp.minimum(a1 - acumt_s[h1:h1 + 1, :], 0.0)), 0.0) * g
            dt = jnp.where(low, dt_s[:, h0:h0 + 1], dt_s[:, h1:h1 + 1])
            x = x_act[:, cols]
            xd = x * dt
            both = jnp.concatenate([m0, m1], axis=1)
            split = jnp.concatenate([jnp.where(low, xd, 0.0), jnp.where(low, 0.0, xd)], axis=0)
            y = jnp.dot(both, split, precision=HI, preferred_element_type=F32)
            ap = jnp.where(low, a0, a1)
            last = jnp.where(low_row, acum_s[T - 1:T, h0:h0 + 1], acum_s[T - 1:T, h1:h1 + 1])
            y = y + cs_buf[:, cols] * jnp.exp(ap)
            xt = xd * jnp.exp(last - ap)
            s_buf[:, cols] = s_buf[:, cols] * jnp.exp(last) + jnp.dot(bt, xt, precision=HI, preferred_element_type=F32)
            y = y + dsk_s[l, :, cols] * x
            z = zd_buf[:, 128 + 128 * p:256 + 128 * p]
            v = y * (z * jax.nn.sigmoid(z))
            v_buf[:, cols] = v
            sq = sq + v * v
        return sq

    first_pairs = (n_pairs + 1) // 2

    def scan_a(j):
        sq_s[...] = scan_pairs(j, range(first_pairs))

    def scan_b(j):
        l, _ = split_item(j)
        sq = sq_s[...] + scan_pairs(j, range(first_pairs, n_pairs))
        ones = jnp.ones((8, 128), F32)
        part = lax.dot_general(ones, sq, (((1,), (1,)), ((), ())), precision=HI, preferred_element_type=F32)
        stats[j, 0:1, :] = part[0:1, :]
        for r in range(len(relations)):
            stat_copy(r, j).start()
        own = lax.rsqrt(jnp.sum(sq, axis=1, keepdims=True) * (1.0 / width) + EPS)
        for p in range(n_pairs):
            cols = slice(128 * p, 128 * (p + 1))
            g_buf[:, cols] = (v_buf[:, cols] * own * gate_s[l, :, cols]).astype(BF16)

    def out_proj(j, h):
        l, c = split_item(j)
        if h == 0:
            @pl.when(c == 0)
            def _():
                out_weight_copy(l).wait()

        g = g_buf[...]
        for n in range(h * half, (h + 1) * half, 256):
            p_buf[:, n:n + 256] = jnp.dot(g, w_o[l, :, n:n + 256], preferred_element_type=F32)
        rdma(0, j, h).start()

    def store_factor(k, wanted, held):
        f_s[k] = jnp.broadcast_to(wanted / jnp.maximum(held, 1e-30), (T, T)).T

    def chip_factors(j):
        wait_stats(j, 0)
        st = stats[j, 0:2, :]
        chip = lax.rsqrt((st[0:1, :] + st[1:2, :]) * (0.5 / width) + EPS)
        for k in range(2):
            store_factor(k, chip, lax.rsqrt(st[k:k + 1, :] * (1.0 / width) + EPS))

    def total_factors(j):
        wait_stats(j, 1)
        st = stats[j]
        rs = lax.rsqrt(jnp.sum(st, axis=0, keepdims=True) * (1.0 / inner_width) + EPS)
        for k, row in ((2, 0), (3, 4), (4, 2)):
            store_factor(k, rs, lax.rsqrt((st[row:row + 1, :] + st[row + 1:row + 2, :]) * (0.5 / width) + EPS))

    def ev1(j, h, first):
        _, c = split_item(j)
        if first:
            chip_factors(j)
        mine = core * (T // 2)
        rdma(0, j, h).wait()

        def add(off):
            f_me = f_s[0, at(mine + off, 16), :]
            f_peer = f_s[1, at(mine + off, 16), :]
            for n in range(h * half, (h + 1) * half, 128):
                cols = slice(n, n + 128)
                r0[c, at(off, 16), cols] = r0[c, at(off, 16), cols] * f_peer + p_buf[at(mine + off, 16), cols] * f_me

        add((1 - xi) * 16)
        rdma(1, j, h).start()
        add(32 + (1 - yi) * 16)
        rdma(2, j, h).start()
        add(xi * 16)
        add(32 + yi * 16)

    def ev2(j, h, first):
        _, c = split_item(j)
        mine = core * (T // 2)
        if first:
            total_factors(j)
        wait_pair(1, j, h)

        def combine(ref, k, off):
            f_own = f_s[2, at(mine + off, 16), :]
            f_other = f_s[k, at(mine + off, 16), :]
            for n in range(h * half, (h + 1) * half, 128):
                cols = slice(n, n + 128)
                ref[c, :, cols] = ref[c, :, cols] * f_other + r0[c, at(off, 16), cols] * f_own

        combine(r1a, 3, xi * 16)
        rdma(3, j, h).start()
        combine(r1b, 4, 32 + yi * 16)
        rdma(4, j, h).start()

    def ev3(j, h, first):
        l, c = split_item(j)
        cols = halves[h]
        base = c * T + core * (T // 2)
        rows_a = at(base + xi * 16 + yi * 8, 8)
        rows_b = at(base + 32 + yi * 16 + xi * 8, 8)
        wait_pair(3, j, h)
        val = r2a[c, :, cols] + r1a[c, at(yi * 8, 8), cols]
        u_buf[slot_of(l + 1), rows_a, cols] = (u_buf[slot_of(l), rows_a, cols] + val).astype(BF16).astype(F32)
        rdma(5, j, h).start()
        val = r2b[c, :, cols] + r1b[c, at(xi * 8, 8), cols]
        u_buf[slot_of(l + 1), rows_b, cols] = (u_buf[slot_of(l), rows_b, cols] + val).astype(BF16).astype(F32)
        rdma(6, j, h).start()

    def ev4(j, h, first):
        wait_pair(5, j, h)
        rdma(7, j, h).start()
        rdma(8, j, h).start()

    def ev5(j, h, first):
        wait_pair(7, j, h)
        rdma(9, j, h).start()

    def ev6(j, h, first):
        l, c = split_item(j)
        rdma(9, j, h).wait()

        def finish():
            @pl.loop(0, T // 16)
            def _(i):
                rows = at(c * T + i * 16, 16, 16)
                out_ref[0, rows, halves[h]] = u_buf[n_layers % 2, rows, halves[h]].astype(BF16)

        if isinstance(j, int):
            if l == n_layers - 1:
                finish()
        else:
            pl.when(l == n_layers - 1)(finish)

    steps = {1: ev1, 2: ev2, 3: ev3, 4: ev4, 5: ev5, 6: ev6}

    def run_step(step, item, h, first):
        with jax.named_scope("ev%d%d" % (step, h)):
            steps[step](item, h, first)

    def slot(k, j):
        for step, h, delta, first, only, skip in SLOTS[k]:
            if only:
                for item in only:
                    pl.when(j == item + delta)(functools.partial(run_step, step, item, h, first))
            else:
                item = j - delta
                there = jnp.logical_and(item >= 0, item < n_items)
                for other in skip:
                    there = jnp.logical_and(there, item != other)
                pl.when(there)(functools.partial(run_step, step, item, h, first))

    pl.semaphore_wait(barrier, len(relations))

    pieces = (in_norm, in_conv, in_gate, scan_prep, scan_a, scan_b, functools.partial(out_proj, h=0),
              functools.partial(out_proj, h=1))
    names = ("norm", "conv", "gate", "prep", "scan_a", "scan_b", "out0", "out1")

    @pl.loop(0, n_items)
    def _(j):
        for k, (piece, name) in enumerate(zip(pieces, names)):
            slot(k, j)

            @pl.when(jnp.logical_and(j >= 0, j < n_items))
            def _():
                with jax.named_scope(name):
                    piece(j)

        slot(len(pieces), j)

    for step, h, item, first in DRAIN:
        run_step(step, item, h, first)


def solution(mesh):
    tp_size = mesh.shape['tp']
    rep_spec = P()
    col_spec = P(None, None, 'tp')
    vec_spec = P(None, 'tp')
    in_specs = (P('dp'), rep_spec, col_spec, col_spec, rep_spec, col_spec, col_spec, rep_spec, vec_spec, rep_spec,
                vec_spec, vec_spec, vec_spec, vec_spec, P(None, 'tp', None))

    def device_forward(hidden, norm_w, w_z, w_x, w_bc, w_dt, conv_x, conv_bc, bias_x, bias_bc, dt_bias, a_log,
                       d_skip, gate_w, w_out):
        n_layers, d_model = norm_w.shape
        n_tok = hidden.shape[1]
        width = w_x.shape[-1]
        n_heads = dt_bias.shape[-1]
        conv_w = width + 2 * STATE
        n_chunks = n_tok // T
        n_items = n_layers * n_chunks
        any_spec = pl.BlockSpec(memory_space=pltpu.HBM)
        vmem_spec = pl.BlockSpec(memory_space=pltpu.VMEM)
        dma = pltpu.SemaphoreType.DMA
        return pl.pallas_call(
            functools.partial(mixer_kernel, n_layers, n_chunks, width * tp_size),
            out_shape=jax.ShapeDtypeStruct(hidden.shape, BF16),
            in_specs=[any_spec] * 15,
            out_specs=vmem_spec,
            scratch_shapes=[
                pltpu.VMEM(norm_w.shape, BF16),
                pltpu.VMEM(conv_x.shape, BF16),
                pltpu.VMEM(conv_bc.shape, BF16),
                pltpu.VMEM(bias_x.shape, BF16),
                pltpu.VMEM(bias_bc.shape, BF16),
                pltpu.VMEM(dt_bias.shape, F32),
                pltpu.VMEM(a_log.shape, F32),
                pltpu.VMEM(d_skip.shape, F32),
                pltpu.VMEM(gate_w.shape, BF16),
                pltpu.VMEM((n_layers, d_model, conv_w + 128 + width), BF16),
                pltpu.VMEM((n_layers, width, d_model), BF16),
                pltpu.VMEM((n_heads, n_layers, d_model), BF16),
                pltpu.VMEM((16 * n_layers, d_model), F32),
                pltpu.VMEM((n_tok, d_model), BF16),
                pltpu.VMEM((2, n_tok, d_model), F32),
                pltpu.VMEM((T, d_model), F32),
                pltpu.VMEM((n_chunks, T // 2, d_model), F32),
                pltpu.VMEM((n_chunks, 16, d_model), F32),
                pltpu.VMEM((n_chunks, 16, d_model), F32),
                pltpu.VMEM((n_chunks, 8, d_model), F32),
                pltpu.VMEM((n_chunks, 8, d_model), F32),
                pltpu.VMEM((T, d_model), BF16),
                pltpu.VMEM((T + 8, conv_w), F32),
                pltpu.VMEM((T, 128 + width), F32),
                pltpu.VMEM((T, width), F32),
                pltpu.VMEM((T, width), F32),
                pltpu.VMEM((T, width), BF16),
                pltpu.VMEM((STATE, width), F32),
                pltpu.VMEM((T, width), F32),
                pltpu.VMEM((T, 128), F32),
                pltpu.VMEM((128, T), F32),
                pltpu.VMEM((T, 128), F32),
                pltpu.VMEM((T, T), F32),
                pltpu.VMEM((STATE, T), F32),
                pltpu.VMEM((T, 128), F32),
                pltpu.VMEM((5, T, T), F32),
                pltpu.VMEM((n_items, 8, T), F32),
                pltpu.VMEM((n_layers, 1, d_model), F32),
                pltpu.VMEM((n_layers, 4, conv_w), F32),
                pltpu.VMEM((n_layers, 1, conv_w), F32),
                pltpu.VMEM((n_layers, 1, 128), F32),
                pltpu.VMEM((n_layers, 1, 128), F32),
                pltpu.VMEM((n_layers, 1, width), F32),
                pltpu.VMEM((n_layers, 1, width), F32),
                dma((n_layers, 3)),
                dma((3,)),
                dma((9,)),
                dma((n_chunks, 2, 6)),
                dma((n_chunks, 2, 6)),
                dma((n_chunks, 2)),
                dma((n_chunks, 2)),
            ],
            compiler_params=pltpu.CompilerParams(
                collective_id=0, has_side_effects=True, vmem_limit_bytes=50000000),
            name="mixer",
        )(*[pltpu.with_memory_space_constraint(arg, pltpu.HBM) for arg in (
            hidden, norm_w, w_z, w_x, w_bc, jnp.transpose(w_dt, (2, 0, 1)), conv_x, conv_bc, bias_x, bias_bc, dt_bias,
            a_log, d_skip, gate_w, w_out)])

    return jax.shard_map(device_forward, mesh=mesh, in_specs=in_specs, out_specs=P('dp'), check_vma=False)
```
